32 devices in a mesh: doc: 2 (over x), seq: 4 (over y, core), head: 4 (over z).
Axes of the slice: x: 2, y: 2, z: 4, core: 2. Of those that a mesh axis runs over, the one named last changes fastest.
Arguments:
- length: int32 [2], P('doc'), parts along dimension 0, may hold values from 896 to 1024
- residual: bfloat16 [2048, 4096], P(('doc', 'seq'), 'head'), parts along dimension 0, may hold values from -6 to 6
- ssm_input: bfloat16 [2048, 4096], P(('doc', 'seq'), 'head'), parts along dimension 0, may hold values from -6 to 6
- state_in: bfloat16 [2048, 128], P(('doc', 'seq')), parts along dimension 0, may hold values from -6 to 6
- state_out: bfloat16 [2048, 128], P(('doc', 'seq')), parts along dimension 0, may hold values from -0.5 to 0.5
- step_raw: float32 [128, 1024], P(('doc', 'head'), 'seq'), parts along dimension 0, may hold values from -5 to 2
- decay_rate: float32 [64], P('head'), may hold values from 0 to 1, as said below
- ssm_gain: float32 [4096], P('head'), may hold values from 0.1 to 1.9
- out_weight: bfloat16 [4096, 4096], P('head'), may hold values from -0.09375 to 0.09375
- norm_gain: float32 [4096], replicated, may hold values from 0.1 to 1.9
- query_weight: bfloat16 [4096, 4096], P(None, 'head'), may hold values from -2 to 2
- key_weight: bfloat16 [4096, 1024], P(None, 'head'), may hold values from -3 to 3
- value_weight: bfloat16 [4096, 1024], P(None, 'head'), may hold values from -0.09375 to 0.09375
Outputs:
- layer_out: bfloat16 [2048, 4096], P(('doc', 'seq'), 'head'), parts along dimension 0
- head_out: bfloat16 [2048, 4096], P(('doc', 'seq'), 'head'), parts along dimension 0
The draws below stay inside these ranges and needn't reach their ends.
There are 2 independent parts, one for each index of `doc`. The reference program is written for one: setup_inputs(seed, part) draws one part's arguments, and reference() takes and returns one part's arrays. A program takes and returns all parts, laid end to end along the dimension named above; an argument that names none is the same for every part. Nothing has to cross between parts.
Inputs may be any that keep to these rules, and one draw needn't show every extreme that they name: The document fills positions 0 to length - 1 of the 1024; later positions are padding. `decay_rate`: positive.
All inputs are finite; a program needn't handle non-finite values.
Results may differ from the reference program's by a relative error of at most 0.028.
The reference program's roundings to bfloat16 on the way count: a program that leaves them out, or rounds other values in their place, can miss the bound.
Values may be sent and summed in bfloat16 or wider, within the bound.
A program may use at most 64 MiB of HBM per device.

```python
import jax
import jax.numpy as jnp
from jax import lax

D = 4096
SSM_HEADS = 64
SSM_HDIM = 64
STATE = 128
Q_HEADS = 32
KV_HEADS = 8
HEAD_DIM = 128
TOK_DEV = 256
INNER = 4096
TOKENS = 1024


def draw_step_raw(key, part):
    blocks = TOKENS // TOK_DEV
    base = jax.random.uniform(jax.random.fold_in(key, 31), (SSM_HEADS, blocks, TOK_DEV), jnp.float32, -3.5, 1.0)
    offset = jax.random.uniform(jax.random.fold_in(key, 32), (SSM_HEADS, blocks, 1), jnp.float32, -1.5, 1.0)
    return (base + offset).reshape(SSM_HEADS, TOKENS)


def draw_decay_rate(key, part):
    order = jax.random.permutation(jax.random.fold_in(key, 21), SSM_HEADS)
    slow = order < SSM_HEADS // 2
    spread = jax.random.uniform(jax.random.fold_in(key, 22), (SSM_HEADS,), jnp.float32)
    slow_rate = jnp.exp(jnp.log(0.25 / TOKENS) + spread * jnp.log(12.0))
    fast_rate = jnp.exp(jnp.log(0.05) + spread * jnp.log(20.0))
    return jnp.where(slow, slow_rate, fast_rate)


def query_key_pair(key):
    scale = 1.6 * D ** (-0.5)
    query_part = jnp.clip(jax.random.normal(jax.random.fold_in(key, 11), (D, Q_HEADS * HEAD_DIM), jnp.float32), -6.0, 6.0) * scale
    key_part = jnp.clip(jax.random.normal(jax.random.fold_in(key, 12), (D, KV_HEADS * HEAD_DIM), jnp.float32), -6.0, 6.0) * scale
    return (query_part, key_part)


def draw_query_weight(key, part):
    return query_key_pair(key)[0].astype(jnp.bfloat16)


def draw_key_weight(key, part):
    return query_key_pair(key)[1].astype(jnp.bfloat16)


def levels(stream_key, extent, split, smallest, top_value):
    gain, own = 1.0, jax.random.fold_in(stream_key, 6)
    for dim, blocks in split:
        heights = jnp.exp(jax.random.uniform(jax.random.fold_in(own, dim), (blocks,), jnp.float32, smallest / len(split), top_value / len(split)))
        gain = gain * jnp.repeat(heights, extent[dim] // blocks).reshape([-1 if axis == dim else 1 for axis in range(len(extent))])
    return gain


def centred(rng, extent, scale, reach, shards=(), kind=jnp.bfloat16):
    drawn = scale * jax.random.normal(rng, extent, jnp.float32)
    if shards:
        drawn = drawn * levels(rng, extent, shards, -0.22, 0.18)
    return jnp.clip(drawn, -reach, reach).astype(kind)


def setup_inputs(seed: int = 0, part: int = 0) -> dict:
    key_list = jax.random.split(jax.random.key(seed), 14)
    part_keys = jax.random.split(jax.random.fold_in(key_list[13], part), 14)
    length = jax.random.randint(part_keys[0], (1,), TOKENS - TOK_DEV // 2, TOKENS + 1).astype(jnp.int32)
    residual = centred(part_keys[1], (TOKENS, D), 1.0, 6.0, ((0, 4), (1, 4)))
    ssm_input = centred(part_keys[2], (TOKENS, INNER), 1.0, 6.0, ((0, 4), (1, 4)))
    state_in = centred(part_keys[3], (TOKENS, STATE), 1.0, 6.0, ((0, 4),))
    state_out = centred(part_keys[4], (TOKENS, STATE), STATE ** -0.5, 0.5, ((0, 4),))
    step_raw = draw_step_raw(jax.random.fold_in(jax.random.fold_in(key_list[13], part), 71), part)
    decay_rate = draw_decay_rate(jax.random.fold_in(key_list[13], 71), part)
    ssm_gain = jnp.clip(1.0 + 0.18 * jax.random.normal(key_list[7], (INNER,), jnp.float32), 0.1, 1.9)
    out_weight = centred(key_list[8], (INNER, D), INNER ** -0.5, 0.09375, ((0, 4),))
    norm_gain = jnp.clip(1.0 + 0.18 * jax.random.normal(key_list[9], (D,), jnp.float32), 0.1, 1.9)
    query_weight = draw_query_weight(jax.random.fold_in(key_list[13], 71), part)
    key_weight = draw_key_weight(jax.random.fold_in(key_list[13], 71), part)
    value_weight = centred(key_list[12], (D, KV_HEADS * HEAD_DIM), D ** -0.5, 0.09375, ((1, 4),))
    return dict(length=length, residual=residual, ssm_input=ssm_input, state_in=state_in, state_out=state_out, step_raw=step_raw, decay_rate=decay_rate, ssm_gain=ssm_gain, out_weight=out_weight, norm_gain=norm_gain, query_weight=query_weight, key_weight=key_weight, value_weight=value_weight)


EPSILON = 1e-05
NEG_BIG = -1e+30
HIGHEST = lax.Precision.HIGHEST

def ssd_blocks(ssm_input, state_in, state_out, delta, decay_rate):
    blocks = TOKENS // TOK_DEV
    inputs = ssm_input.astype(jnp.float32).reshape(blocks, TOK_DEV, SSM_HEADS, SSM_HDIM)
    enter = state_in.reshape(blocks, TOK_DEV, STATE)
    leave = state_out.reshape(blocks, TOK_DEV, STATE)
    steps = delta.reshape(SSM_HEADS, blocks, TOK_DEV).transpose(1, 0, 2)
    causal = jnp.arange(TOK_DEV)[:, None] >= jnp.arange(TOK_DEV)[None, :]

    def advance(carried, inputs_now):
        block_in, enter_now, leave_now, step_now = inputs_now
        cumlog = jnp.cumsum(-decay_rate[:, None] * step_now, axis=1)
        inner = jnp.dot(leave_now, enter_now.T, preferred_element_type=jnp.float32)
        spread = cumlog[:, :, None] - cumlog[:, None, :]
        mixing = jnp.where(causal[None], jnp.exp(jnp.where(causal[None], spread, 0.0)), 0.0) * inner[None] * step_now[:, None, :]
        within = jnp.einsum('hts,shp->thp', mixing, block_in, precision=HIGHEST)
        carried_out = jnp.einsum('hpn,tn->thp', carried, leave_now.astype(jnp.float32), precision=HIGHEST)
        output = within + jnp.exp(cumlog).T[:, :, None] * carried_out
        tail = jnp.exp(cumlog[:, -1:] - cumlog) * step_now
        fresh = jnp.einsum('hs,shp,sn->hpn', tail, block_in, enter_now.astype(jnp.float32), precision=HIGHEST)
        following = jnp.exp(cumlog[:, -1])[:, None, None] * carried + fresh
        return (following, output)
    start = jnp.zeros((SSM_HEADS, SSM_HDIM, STATE), jnp.float32)
    unused, outputs = lax.scan(advance, start, (inputs, enter, leave, steps))
    return outputs.reshape(TOKENS, SSM_HEADS, SSM_HDIM)

def reference(length, residual, ssm_input, state_in, state_out, step_raw, decay_rate, ssm_gain, out_weight, norm_gain, query_weight, key_weight, value_weight):
    positions = jnp.arange(TOKENS, dtype=jnp.int32)
    live_rows = positions < length[0]
    live = live_rows.astype(jnp.float32)
    delta = live[None, :] * jax.nn.softplus(step_raw)
    ssm_out = ssd_blocks(ssm_input, state_in, state_out, delta, decay_rate) * live[:, None, None]
    mean_square = lax.optimization_barrier(jnp.mean(ssm_out * ssm_out, axis=2, keepdims=True))
    normed = (ssm_out * lax.rsqrt(mean_square + EPSILON) * ssm_gain.reshape(SSM_HEADS, SSM_HDIM)).astype(jnp.bfloat16)
    normed = normed.reshape(TOKENS, SSM_HEADS * SSM_HDIM)
    projected = jnp.dot(normed, out_weight, preferred_element_type=jnp.float32)
    layer_out = (residual.astype(jnp.float32) + projected).astype(jnp.bfloat16)
    widened = layer_out.astype(jnp.float32)
    attn_in = (widened * lax.rsqrt(lax.optimization_barrier(jnp.mean(widened * widened, axis=1, keepdims=True)) + EPSILON) * norm_gain).astype(jnp.bfloat16)
    queries = jnp.dot(attn_in, query_weight, preferred_element_type=jnp.float32).astype(jnp.bfloat16)
    keys = jnp.dot(attn_in, key_weight, preferred_element_type=jnp.float32).astype(jnp.bfloat16)
    values = jnp.dot(attn_in, value_weight, preferred_element_type=jnp.float32).astype(jnp.bfloat16)
    group_size = Q_HEADS // KV_HEADS
    query_heads = queries.reshape(TOKENS, Q_HEADS, HEAD_DIM).transpose(1, 0, 2)
    key_heads = jnp.repeat(keys.reshape(TOKENS, KV_HEADS, HEAD_DIM).transpose(1, 0, 2), group_size, axis=0)
    value_heads = jnp.repeat(values.reshape(TOKENS, KV_HEADS, HEAD_DIM).transpose(1, 0, 2), group_size, axis=0)
    allowed = (positions[None, :] <= positions[:, None]) & live_rows[None, :]

    def one_head(operands):
        query_now, key_now, value_now = operands
        scores = jnp.dot(query_now, key_now.T, preferred_element_type=jnp.float32) * HEAD_DIM ** (-0.5)
        masked = jnp.where(allowed, scores, NEG_BIG)
        best = lax.optimization_barrier(jnp.max(masked, axis=1, keepdims=True))
        weights = jnp.where(allowed, jnp.exp(masked - best), 0.0)
        total = lax.optimization_barrier(jnp.sum(weights, axis=1, keepdims=True))
        mixed = jnp.dot(weights.astype(jnp.bfloat16), value_now, preferred_element_type=jnp.float32)
        return mixed / jnp.where(live_rows[:, None], total, 1.0) * live[:, None]
    heads = lax.map(one_head, (query_heads, key_heads, value_heads))
    head_out = heads.transpose(1, 0, 2).reshape(TOKENS, Q_HEADS * HEAD_DIM).astype(jnp.bfloat16)
    return (layer_out, head_out)
```

```python
import jax
import jax.numpy as jnp
from jax import lax
from jax.sharding import PartitionSpec as P

HEAD_DIM = 128


EPSILON = 1e-05
NEG_BIG = -1e30
HIGHEST = lax.Precision.HIGHEST


def split_3(value):
    high = lax.reduce_precision(value, 8, 7)
    middle = lax.reduce_precision(value - high, 8, 7)
    low = value - high - middle
    return jnp.stack([high, middle, low], axis=1).astype(jnp.bfloat16)


def incoming_state(log_decay, local_state, axis):
    count, mine = (lax.axis_size(axis), lax.axis_index(axis))
    heads, width, states = local_state.shape
    decay_rows = jnp.pad(split_3(log_decay), ((0, 0), (0, states - 3)))
    packed = jnp.concatenate(
        [local_state.astype(jnp.bfloat16).reshape(heads * width, states), decay_rows], axis=0
    )
    pieces = lax.all_gather(packed, axis)
    logs = jnp.sum(pieces[:, heads * width :, :3].astype(jnp.float32), axis=2)
    order = jnp.arange(count)
    between = (order[None, :] > order[:, None]) & (order[None, :] < mine)
    reach = jnp.sum(jnp.where(between[:, :, None], logs[None], 0.0), axis=1)
    factor = jnp.where((order < mine)[:, None], jnp.exp(reach), 0.0)
    total = jnp.zeros(local_state.shape, jnp.float32)
    for position in range(count - 1):
        piece = pieces[position, : heads * width].reshape(heads, width, states)
        total += factor[position][:, None, None] * piece.astype(jnp.float32)
    return total


def chain_scatter(partial_value, axis):
    count, mine = (lax.axis_size(axis), lax.axis_index(axis))
    width = partial_value.shape[1] // count

    def block(index):
        start = jnp.clip(index, 0, count - 1) * width
        return lax.dynamic_slice_in_dim(partial_value, start, width, axis=1)

    up = down = None
    for step in range(count - 1):
        own_up = block(count - 1 - step + mine)
        own_down = block(step - (count - 1 - mine))
        send_up = own_up if up is None else own_up + up.astype(jnp.float32)
        send_down = own_down if down is None else own_down + down.astype(jnp.float32)
        up = lax.ppermute(
            send_up.astype(jnp.bfloat16), axis, [(z, z + 1) for z in range(step + 1)]
        )
        down = lax.ppermute(
            send_down.astype(jnp.bfloat16),
            axis,
            [(count - 1 - z, count - 2 - z) for z in range(step + 1)],
        )
    total = block(mine)
    if up is not None:
        total = total + up.astype(jnp.float32) + down.astype(jnp.float32)
    return total


def body(
    length,
    residual,
    ssm_input,
    state_in,
    state_out,
    step_raw,
    decay_rate,
    ssm_gain,
    out_weight,
    norm_gain,
    query_weight,
    key_weight,
    value_weight,
):
    rows = residual.shape[0]
    local_heads = decay_rate.shape[0]
    head_width = ssm_input.shape[1] // local_heads
    seq_index = lax.axis_index("seq")
    limit = length[0]
    positions = seq_index * rows + jnp.arange(rows, dtype=jnp.int32)
    live_rows = positions < limit
    live = live_rows.astype(jnp.float32)
    delta = live[None, :] * jax.nn.softplus(step_raw)
    cumlog = jnp.cumsum(-decay_rate[:, None] * delta, axis=1)
    inputs = ssm_input.astype(jnp.float32).reshape(rows, local_heads, head_width)
    inner = jnp.dot(state_out, state_in.T, preferred_element_type=jnp.float32)
    causal = jnp.arange(rows)[:, None] >= jnp.arange(rows)[None, :]
    spread = cumlog[:, :, None] - cumlog[:, None, :]
    mixing = (
        jnp.where(causal[None], jnp.exp(jnp.where(causal[None], spread, 0.0)), 0.0)
        * inner[None]
        * delta[:, None, :]
    )
    within = jnp.einsum("hts,shp->thp", mixing, inputs, precision=HIGHEST)
    tail = jnp.exp(cumlog[:, -1:] - cumlog) * delta
    local_state = jnp.einsum(
        "hs,shp,sn->hpn", tail, inputs, state_in.astype(jnp.float32), precision=HIGHEST
    )
    incoming = incoming_state(cumlog[:, -1], local_state, "seq")
    carried = jnp.einsum("hpn,tn->thp", incoming, state_out.astype(jnp.float32), precision=HIGHEST)
    ssm_out = (within + jnp.exp(cumlog).T[:, :, None] * carried) * live[:, None, None]
    mean_square = jnp.mean(ssm_out * ssm_out, axis=2, keepdims=True)
    normed = (
        ssm_out * lax.rsqrt(mean_square + EPSILON) * ssm_gain.reshape(local_heads, head_width)
    ).astype(jnp.bfloat16)
    normed = normed.reshape(rows, local_heads * head_width)
    partial_value = jnp.dot(normed, out_weight, preferred_element_type=jnp.float32)
    projected = chain_scatter(partial_value, "head")
    layer_out = (residual.astype(jnp.float32) + projected).astype(jnp.bfloat16)
    widened = lax.all_gather(layer_out, "head", axis=1, tiled=True).astype(jnp.float32)
    squares = jnp.mean(widened * widened, axis=1, keepdims=True)
    attn_in = (widened * lax.rsqrt(squares + EPSILON) * norm_gain).astype(jnp.bfloat16)
    queries = jnp.dot(attn_in, query_weight, preferred_element_type=jnp.float32).astype(
        jnp.bfloat16
    )
    keys = jnp.dot(attn_in, key_weight, preferred_element_type=jnp.float32).astype(jnp.bfloat16)
    values = jnp.dot(attn_in, value_weight, preferred_element_type=jnp.float32).astype(jnp.bfloat16)
    query_local = query_weight.shape[1] // HEAD_DIM
    kv_local = key_weight.shape[1] // HEAD_DIM
    group_size = query_local // kv_local
    grouped = queries.reshape(rows, kv_local, group_size, HEAD_DIM)
    best = jnp.full((rows, query_local), NEG_BIG, jnp.float32)
    key_value = lax.all_gather(
        jnp.concatenate([keys, values], axis=1), "seq", axis=0, tiled=True
    )
    key_piece = key_value[:, : keys.shape[1]]
    value_piece = key_value[:, keys.shape[1] :]
    count = key_piece.shape[0]
    key_pos = jnp.arange(count, dtype=jnp.int32)
    allowed = (key_pos[None, :] <= positions[:, None]) & (key_pos[None, :] < limit)
    scores = jnp.einsum(
        "tkgd,rkd->tkgr",
        grouped,
        key_piece.reshape(count, kv_local, HEAD_DIM),
        preferred_element_type=jnp.float32,
    ) * HEAD_DIM ** (-0.5)
    scores = scores.reshape(rows, query_local, count)
    allowed_wide = allowed[:, None, :]
    masked = jnp.where(allowed_wide, scores, NEG_BIG)
    new_best = jnp.maximum(best, jnp.max(masked, axis=2))
    weights = jnp.where(allowed_wide, jnp.exp(masked - new_best[:, :, None]), 0.0)
    total = jnp.sum(weights, axis=2)
    update = jnp.einsum(
        "tkgr,rkd->tkgd",
        weights.astype(jnp.bfloat16).reshape(rows, kv_local, group_size, count),
        value_piece.reshape(count, kv_local, HEAD_DIM),
        preferred_element_type=jnp.float32,
    )
    accum = update.reshape(rows, query_local, HEAD_DIM)
    folded = (new_best, total, accum)
    total = folded[1]
    accum = folded[2]
    safe_total = jnp.where(live_rows[:, None], total, 1.0)
    head_out = (
        (accum / safe_total[:, :, None] * live[:, None, None])
        .astype(jnp.bfloat16)
        .reshape(rows, query_local * HEAD_DIM)
    )
    return (layer_out, head_out)


def solution(mesh):
    placed = (
        P("doc"),
        P(("doc", "seq"), "head"),
        P(("doc", "seq"), "head"),
        P(("doc", "seq"), None),
        P(("doc", "seq"), None),
        P(("doc", "head"), "seq"),
        P("head"),
        P("head"),
        P("head", None),
        P(),
        P(None, "head"),
        P(None, "head"),
        P(None, "head"),
    )
    return jax.shard_map(
        body,
        mesh=mesh,
        in_specs=placed,
        out_specs=(P(("doc", "seq"), "head"), P(("doc", "seq"), "head")),
        check_vma=False,
    )
```

```python
import functools

import jax
import jax.numpy as jnp
from jax import lax
from jax.experimental import pallas as pl
from jax.experimental.pallas import tpu as pltpu
from jax.sharding import PartitionSpec as P

HEAD_DIM = 128


EPSILON = 1e-05
NEG_BIG = -1e30
HIGHEST = lax.Precision.HIGHEST


def split_3(value):
    high = lax.reduce_precision(value, 8, 7)
    middle = lax.reduce_precision(value - high, 8, 7)
    low = value - high - middle
    return jnp.stack([high, middle, low], axis=1).astype(jnp.bfloat16)


def incoming_state(log_decay, local_state, axis):
    count, mine = (lax.axis_size(axis), lax.axis_index(axis))
    heads, width, states = local_state.shape
    decay_rows = jnp.pad(split_3(log_decay), ((0, 0), (0, states - 3)))
    packed = jnp.concatenate(
        [local_state.astype(jnp.bfloat16).reshape(heads * width, states), decay_rows], axis=0
    )
    pieces = lax.all_gather(packed, axis)
    logs = jnp.sum(pieces[:, heads * width :, :3].astype(jnp.float32), axis=2)
    order = jnp.arange(count)
    between = (order[None, :] > order[:, None]) & (order[None, :] < mine)
    reach = jnp.sum(jnp.where(between[:, :, None], logs[None], 0.0), axis=1)
    factor = jnp.where((order < mine)[:, None], jnp.exp(reach), 0.0)
    total = jnp.zeros(local_state.shape, jnp.float32)
    for position in range(count - 1):
        piece = pieces[position, : heads * width].reshape(heads, width, states)
        total += factor[position][:, None, None] * piece.astype(jnp.float32)
    return total


def line_kernel(
    count,
    chunks,
    partial_ref,
    residual_ref,
    gain_ref,
    layer_ref,
    attn_ref,
    stage_ref,
    landed_ref,
    gathered_ref,
    total_ref,
    sum_send,
    sum_recv,
    copy_send,
    copy_recv,
):
    mine = lax.axis_index("head")
    last = count - 1
    width = residual_ref.shape[1]
    rows = residual_ref.shape[0] // chunks
    place = (mine, last - mine)

    barrier = pltpu.get_barrier_semaphore()

    def greet(neighbour):
        pl.semaphore_signal(
            barrier, inc=1, device_id={"head": neighbour}, device_id_type=pl.DeviceIdType.MESH
        )

    @pl.when(mine > 0)
    def _():
        greet(mine - 1)

    @pl.when(mine < last)
    def _():
        greet(mine + 1)

    @pl.when((mine == 0) | (mine == last))
    def _():
        pl.semaphore_wait(barrier, 1)

    @pl.when((mine > 0) & (mine < last))
    def _():
        pl.semaphore_wait(barrier, 2)

    def neighbour(way):
        return mine + 1 if way == 0 else mine - 1

    def real(way, position):
        return position if way == 0 else last - position

    def sum_copy(way, chunk, step):
        return pltpu.make_async_remote_copy(
            src_ref=stage_ref.at[way, chunk, step],
            dst_ref=landed_ref.at[way, chunk, step],
            send_sem=sum_send.at[way, chunk, step],
            recv_sem=sum_recv.at[way, chunk, step],
            device_id={"head": neighbour(way)},
            device_id_type=pl.DeviceIdType.MESH,
        )

    def block_copy(way, chunk, step, source):
        block = gathered_ref.at[source, pl.ds(chunk * rows, rows)]
        return pltpu.make_async_remote_copy(
            src_ref=block,
            dst_ref=block,
            send_sem=copy_send.at[way, chunk, step],
            recv_sem=copy_recv.at[way, chunk, step],
            device_id={"head": neighbour(way)},
            device_id_type=pl.DeviceIdType.MESH,
        )

    def own_part(chunk, owner):
        columns = pl.ds(pl.multiple_of(owner * width, 128), width)
        return partial_ref[pl.ds(chunk * rows, rows), columns]

    def sum_step(chunk, step):
        for way in range(2):
            owner = real(way, last - step + place[way])

            @pl.when(place[way] == 0)
            def _():
                stage_ref[way, chunk, step] = own_part(chunk, owner).astype(jnp.bfloat16)
                sum_copy(way, chunk, step).start()

            if step == 0:
                continue

            @pl.when((place[way] <= step) & (place[way] > 0))
            def _():
                sum_copy(way, chunk, step - 1).wait_recv()
                arrived = landed_ref[way, chunk, step - 1].astype(jnp.float32)
                stage_ref[way, chunk, step] = (own_part(chunk, owner) + arrived).astype(
                    jnp.bfloat16
                )
                sum_copy(way, chunk, step).start()

    def finish_sum(chunk):
        here = pl.ds(chunk * rows, rows)
        total_ref[...] = residual_ref[here].astype(jnp.float32) + own_part(chunk, mine)
        for way in range(2):

            @pl.when(place[way] > 0)
            def _():
                sum_copy(way, chunk, last - 1).wait_recv()
                total_ref[...] += landed_ref[way, chunk, last - 1].astype(jnp.float32)

        layer_low = total_ref[...].astype(jnp.bfloat16)
        gathered_ref[mine, here] = layer_low
        layer_ref[here] = layer_low
        for way in range(2):

            @pl.when(place[way] < last)
            def _():
                block_copy(way, chunk, 0, mine).start()

    def forward(chunk, step):
        for way in range(2):
            source = real(way, place[way] - step)

            @pl.when(place[way] >= step)
            def _():
                block_copy(way, chunk, step - 1, source).wait_recv()

            @pl.when((place[way] >= step) & (place[way] < last))
            def _():
                block_copy(way, chunk, step, source).start()

    def normalise(chunk):
        for way in range(2):

            @pl.when(place[way] == last)
            def _():
                block_copy(way, chunk, last - 1, real(way, 0)).wait_recv()

        here = pl.ds(chunk * rows, rows)
        squares = jnp.zeros((rows, 1), jnp.float32)
        for source in range(count):
            block = gathered_ref[source, here].astype(jnp.float32)
            squares += jnp.sum(block * block, axis=1, keepdims=True)
        scale = lax.rsqrt(squares / (count * width) + EPSILON)
        for source in range(count):
            columns = slice(source * width, (source + 1) * width)
            block = gathered_ref[source, here].astype(jnp.float32)
            attn_ref[here, columns] = (block * scale * gain_ref[:, columns]).astype(jnp.bfloat16)

    for tick in range(chunks + 2 * last):
        for chunk in range(chunks):
            stage = tick - chunk
            if 0 <= stage < last:
                sum_step(chunk, stage)
            elif stage == last:
                finish_sum(chunk)
            elif last < stage < 2 * last:
                forward(chunk, stage - last)
            elif stage == 2 * last:
                normalise(chunk)

    for chunk in range(chunks):
        for step in range(last):
            for way in range(2):

                @pl.when(place[way] <= step)
                def _():
                    sum_copy(way, chunk, step).wait_send()

                @pl.when((place[way] >= step) & (place[way] < last))
                def _():
                    block_copy(way, chunk, step, real(way, place[way] - step)).wait_send()


def line_sum_and_gather(partial_value, residual, norm_gain, count):
    rows, width = residual.shape
    chunks = 4 if rows % 64 == 0 else 1
    steps = count - 1
    piece = rows // chunks
    messages = (2, chunks, steps)
    return pl.pallas_call(
        functools.partial(line_kernel, count, chunks),
        out_shape=(
            jax.ShapeDtypeStruct((rows, width), jnp.bfloat16),
            jax.ShapeDtypeStruct((rows, width * count), jnp.bfloat16),
        ),
        in_specs=[pl.BlockSpec(memory_space=pltpu.VMEM)] * 3,
        out_specs=[pl.BlockSpec(memory_space=pltpu.VMEM)] * 2,
        scratch_shapes=[
            pltpu.VMEM(messages + (piece, width), jnp.bfloat16),
            pltpu.VMEM(messages + (piece, width), jnp.bfloat16),
            pltpu.VMEM((count, rows, width), jnp.bfloat16),
            pltpu.VMEM((piece, width), jnp.float32),
            pltpu.SemaphoreType.DMA(messages),
            pltpu.SemaphoreType.DMA(messages),
            pltpu.SemaphoreType.DMA(messages),
            pltpu.SemaphoreType.DMA(messages),
        ],
        compiler_params=pltpu.CompilerParams(
            collective_id=0, has_side_effects=True, vmem_limit_bytes=40 * 1024 * 1024
        ),
    )(partial_value, residual, norm_gain.reshape(1, width * count))


def body(
    length,
    residual,
    ssm_input,
    state_in,
    state_out,
    step_raw,
    decay_rate,
    ssm_gain,
    out_weight,
    norm_gain,
    query_weight,
    key_weight,
    value_weight,
):
    rows = residual.shape[0]
    local_heads = decay_rate.shape[0]
    head_width = ssm_input.shape[1] // local_heads
    seq_index = lax.axis_index("seq")
    limit = length[0]
    positions = seq_index * rows + jnp.arange(rows, dtype=jnp.int32)
    live_rows = positions < limit
    live = live_rows.astype(jnp.float32)
    delta = live[None, :] * jax.nn.softplus(step_raw)
    cumlog = jnp.cumsum(-decay_rate[:, None] * delta, axis=1)
    inputs = ssm_input.astype(jnp.float32).reshape(rows, local_heads, head_width)
    inner = jnp.dot(state_out, state_in.T, preferred_element_type=jnp.float32)
    causal = jnp.arange(rows)[:, None] >= jnp.arange(rows)[None, :]
    spread = cumlog[:, :, None] - cumlog[:, None, :]
    mixing = (
        jnp.where(causal[None], jnp.exp(jnp.where(causal[None], spread, 0.0)), 0.0)
        * inner[None]
        * delta[:, None, :]
    )
    within = jnp.einsum("hts,shp->thp", mixing, inputs, precision=HIGHEST)
    tail = jnp.exp(cumlog[:, -1:] - cumlog) * delta
    local_state = jnp.einsum(
        "hs,shp,sn->hpn", tail, inputs, state_in.astype(jnp.float32), precision=HIGHEST
    )
    incoming = incoming_state(cumlog[:, -1], local_state, "seq")
    carried = jnp.einsum("hpn,tn->thp", incoming, state_out.astype(jnp.float32), precision=HIGHEST)
    ssm_out = (within + jnp.exp(cumlog).T[:, :, None] * carried) * live[:, None, None]
    mean_square = jnp.mean(ssm_out * ssm_out, axis=2, keepdims=True)
    normed = (
        ssm_out * lax.rsqrt(mean_square + EPSILON) * ssm_gain.reshape(local_heads, head_width)
    ).astype(jnp.bfloat16)
    normed = normed.reshape(rows, local_heads * head_width)
    partial_value = jnp.dot(normed, out_weight, preferred_element_type=jnp.float32)
    layer_out, attn_in = line_sum_and_gather(
        partial_value, residual, norm_gain, lax.axis_size("head")
    )
    queries = jnp.dot(attn_in, query_weight, preferred_element_type=jnp.float32).astype(
        jnp.bfloat16
    )
    keys = jnp.dot(attn_in, key_weight, preferred_element_type=jnp.float32).astype(jnp.bfloat16)
    values = jnp.dot(attn_in, value_weight, preferred_element_type=jnp.float32).astype(jnp.bfloat16)
    query_local = query_weight.shape[1] // HEAD_DIM
    kv_local = key_weight.shape[1] // HEAD_DIM
    group_size = query_local // kv_local
    grouped = queries.reshape(rows, kv_local, group_size, HEAD_DIM)
    best = jnp.full((rows, query_local), NEG_BIG, jnp.float32)
    key_value = lax.all_gather(
        jnp.concatenate([keys, values], axis=1), "seq", axis=0, tiled=True
    )
    key_piece = key_value[:, : keys.shape[1]]
    value_piece = key_value[:, keys.shape[1] :]
    count = key_piece.shape[0]
    key_pos = jnp.arange(count, dtype=jnp.int32)
    allowed = (key_pos[None, :] <= positions[:, None]) & (key_pos[None, :] < limit)
    scores = jnp.einsum(
        "tkgd,rkd->tkgr",
        grouped,
        key_piece.reshape(count, kv_local, HEAD_DIM),
        preferred_element_type=jnp.float32,
    ) * HEAD_DIM ** (-0.5)
    scores = scores.reshape(rows, query_local, count)
    allowed_wide = allowed[:, None, :]
    masked = jnp.where(allowed_wide, scores, NEG_BIG)
    new_best = jnp.maximum(best, jnp.max(masked, axis=2))
    weights = jnp.where(allowed_wide, jnp.exp(masked - new_best[:, :, None]), 0.0)
    total = jnp.sum(weights, axis=2)
    update = jnp.einsum(
        "tkgr,rkd->tkgd",
        weights.astype(jnp.bfloat16).reshape(rows, kv_local, group_size, count),
        value_piece.reshape(count, kv_local, HEAD_DIM),
        preferred_element_type=jnp.float32,
    )
    accum = update.reshape(rows, query_local, HEAD_DIM)
    folded = (new_best, total, accum)
    total = folded[1]
    accum = folded[2]
    safe_total = jnp.where(live_rows[:, None], total, 1.0)
    head_out = (
        (accum / safe_total[:, :, None] * live[:, None, None])
        .astype(jnp.bfloat16)
        .reshape(rows, query_local * HEAD_DIM)
    )
    return (layer_out, head_out)


def solution(mesh):
    placed = (
        P("doc"),
        P(("doc", "seq"), "head"),
        P(("doc", "seq"), "head"),
        P(("doc", "seq"), None),
        P(("doc", "seq"), None),
        P(("doc", "head"), "seq"),
        P("head"),
        P("head"),
        P("head", None),
        P(),
        P(None, "head"),
        P(None, "head"),
        P(None, "head"),
    )
    return jax.shard_map(
        body,
        mesh=mesh,
        in_specs=placed,
        out_specs=(P(("doc", "seq"), "head"), P(("doc", "seq"), "head")),
        check_vma=False,
    )
```

```python
import functools

import jax
import jax.numpy as jnp
from jax import lax
from jax.experimental import pallas as pl
from jax.experimental.pallas import tpu as pltpu
from jax.sharding import PartitionSpec as P

HEAD_DIM = 128


EPSILON = 1e-05
NEG_BIG = -1e30
HIGHEST = lax.Precision.HIGHEST


def split_3(value):
    high = lax.reduce_precision(value, 8, 7)
    middle = lax.reduce_precision(value - high, 8, 7)
    low = value - high - middle
    return jnp.stack([high, middle, low], axis=1).astype(jnp.bfloat16)


def incoming_state(log_decay, local_state, axis):
    count, mine = (lax.axis_size(axis), lax.axis_index(axis))
    heads, width, states = local_state.shape
    decay_rows = jnp.pad(split_3(log_decay), ((0, 0), (0, states - 3)))
    packed = jnp.concatenate(
        [local_state.astype(jnp.bfloat16).reshape(heads * width, states), decay_rows], axis=0
    )
    pieces = lax.all_gather(packed, axis)
    logs = jnp.sum(pieces[:, heads * width :, :3].astype(jnp.float32), axis=2)
    order = jnp.arange(count)
    between = (order[None, :] > order[:, None]) & (order[None, :] < mine)
    reach = jnp.sum(jnp.where(between[:, :, None], logs[None], 0.0), axis=1)
    factor = jnp.where((order < mine)[:, None], jnp.exp(reach), 0.0)
    total = jnp.zeros(local_state.shape, jnp.float32)
    for position in range(count - 1):
        piece = pieces[position, : heads * width].reshape(heads, width, states)
        total += factor[position][:, None, None] * piece.astype(jnp.float32)
    return total


def line_kernel(
    count,
    chunks,
    partial_ref,
    residual_ref,
    gain_ref,
    layer_ref,
    attn_ref,
    stage_ref,
    landed_ref,
    gathered_ref,
    total_ref,
    sum_send,
    sum_recv,
    copy_send,
    copy_recv,
):
    mine = lax.axis_index("head")
    last = count - 1
    width = residual_ref.shape[1]
    rows = residual_ref.shape[0] // chunks
    place = (mine, last - mine)

    barrier = pltpu.get_barrier_semaphore()

    def greet(neighbour):
        pl.semaphore_signal(
            barrier, inc=1, device_id={"head": neighbour}, device_id_type=pl.DeviceIdType.MESH
        )

    @pl.when(mine > 0)
    def _():
        greet(mine - 1)

    @pl.when(mine < last)
    def _():
        greet(mine + 1)

    @pl.when((mine == 0) | (mine == last))
    def _():
        pl.semaphore_wait(barrier, 1)

    @pl.when((mine > 0) & (mine < last))
    def _():
        pl.semaphore_wait(barrier, 2)

    def neighbour(way):
        return mine + 1 if way == 0 else mine - 1

    def real(way, position):
        return position if way == 0 else last - position

    def sum_copy(way, chunk, step):
        return pltpu.make_async_remote_copy(
            src_ref=stage_ref.at[way, chunk, step],
            dst_ref=landed_ref.at[way, chunk, step],
            send_sem=sum_send.at[way, chunk, step],
            recv_sem=sum_recv.at[way, chunk, step],
            device_id={"head": neighbour(way)},
            device_id_type=pl.DeviceIdType.MESH,
        )

    def block_copy(way, chunk, step, source):
        block = gathered_ref.at[source, pl.ds(chunk * rows, rows)]
        return pltpu.make_async_remote_copy(
            src_ref=block,
            dst_ref=block,
            send_sem=copy_send.at[way, chunk, step],
            recv_sem=copy_recv.at[way, chunk, step],
            device_id={"head": neighbour(way)},
            device_id_type=pl.DeviceIdType.MESH,
        )

    def own_part(chunk, owner):
        columns = pl.ds(pl.multiple_of(owner * width, 128), width)
        return partial_ref[pl.ds(chunk * rows, rows), columns]

    def sum_step(chunk, step):
        for way in range(2):
            owner = real(way, last - step + place[way])

            @pl.when(place[way] == 0)
            def _():
                stage_ref[way, chunk, step] = own_part(chunk, owner).astype(jnp.bfloat16)
                sum_copy(way, chunk, step).start()

            if step == 0:
                continue

            @pl.when((place[way] <= step) & (place[way] > 0))
            def _():
                sum_copy(way, chunk, step - 1).wait_recv()
                arrived = landed_ref[way, chunk, step - 1].astype(jnp.float32)
                stage_ref[way, chunk, step] = (own_part(chunk, owner) + arrived).astype(
                    jnp.bfloat16
                )
                sum_copy(way, chunk, step).start()

    def finish_sum(chunk):
        here = pl.ds(chunk * rows, rows)
        total_ref[...] = residual_ref[here].astype(jnp.float32) + own_part(chunk, mine)
        for way in range(2):

            @pl.when(place[way] > 0)
            def _():
                sum_copy(way, chunk, last - 1).wait_recv()
                total_ref[...] += landed_ref[way, chunk, last - 1].astype(jnp.float32)

        layer_low = total_ref[...].astype(jnp.bfloat16)
        gathered_ref[mine, here] = layer_low
        layer_ref[here] = layer_low
        for way in range(2):

            @pl.when(place[way] < last)
            def _():
                block_copy(way, chunk, 0, mine).start()

    def forward(chunk, step):
        for way in range(2):
            source = real(way, place[way] - step)

            @pl.when(place[way] >= step)
            def _():
                block_copy(way, chunk, step - 1, source).wait_recv()

            @pl.when((place[way] >= step) & (place[way] < last))
            def _():
                block_copy(way, chunk, step, source).start()

    def normalise(chunk):
        for way in range(2):

            @pl.when(place[way] == last)
            def _():
                block_copy(way, chunk, last - 1, real(way, 0)).wait_recv()

        here = pl.ds(chunk * rows, rows)
        squares = jnp.zeros((rows, 1), jnp.float32)
        for source in range(count):
            block = gathered_ref[source, here].astype(jnp.float32)
            squares += jnp.sum(block * block, axis=1, keepdims=True)
        scale = lax.rsqrt(squares / (count * width) + EPSILON)
        for source in range(count):
            columns = slice(source * width, (source + 1) * width)
            block = gathered_ref[source, here].astype(jnp.float32)
            attn_ref[here, columns] = (block * scale * gain_ref[:, columns]).astype(jnp.bfloat16)

    for tick in range(chunks + 2 * last):
        for chunk in range(chunks):
            stage = tick - chunk
            if 0 <= stage < last:
                sum_step(chunk, stage)
            elif stage == last:
                finish_sum(chunk)
            elif last < stage < 2 * last:
                forward(chunk, stage - last)
            elif stage == 2 * last:
                normalise(chunk)

    for chunk in range(chunks):
        for step in range(last):
            for way in range(2):

                @pl.when(place[way] <= step)
                def _():
                    sum_copy(way, chunk, step).wait_send()

                @pl.when((place[way] >= step) & (place[way] < last))
                def _():
                    block_copy(way, chunk, step, real(way, place[way] - step)).wait_send()


def line_sum_and_gather(partial_value, residual, norm_gain, count):
    rows, width = residual.shape
    chunks = 8 if rows % 128 == 0 else 1
    steps = count - 1
    piece = rows // chunks
    messages = (2, chunks, steps)
    return pl.pallas_call(
        functools.partial(line_kernel, count, chunks),
        out_shape=(
            jax.ShapeDtypeStruct((rows, width), jnp.bfloat16),
            jax.ShapeDtypeStruct((rows, width * count), jnp.bfloat16),
        ),
        in_specs=[pl.BlockSpec(memory_space=pltpu.VMEM)] * 3,
        out_specs=[pl.BlockSpec(memory_space=pltpu.VMEM)] * 2,
        scratch_shapes=[
            pltpu.VMEM(messages + (piece, width), jnp.bfloat16),
            pltpu.VMEM(messages + (piece, width), jnp.bfloat16),
            pltpu.VMEM((count, rows, width), jnp.bfloat16),
            pltpu.VMEM((piece, width), jnp.float32),
            pltpu.SemaphoreType.DMA(messages),
            pltpu.SemaphoreType.DMA(messages),
            pltpu.SemaphoreType.DMA(messages),
            pltpu.SemaphoreType.DMA(messages),
        ],
        compiler_params=pltpu.CompilerParams(
            collective_id=0, has_side_effects=True, vmem_limit_bytes=40 * 1024 * 1024
        ),
    )(partial_value, residual, norm_gain.reshape(1, width * count))


def attention_kernel(group_size, limits_ref, query_ref, key_ref, value_ref, out_ref):
    rows, count = query_ref.shape[0], key_ref.shape[0]
    limit, first = limits_ref[0], limits_ref[1]
    key_pos = lax.broadcasted_iota(jnp.int32, (rows, count), 1)
    positions = first + lax.broadcasted_iota(jnp.int32, (rows, count), 0)
    allowed = (key_pos <= positions) & (key_pos < limit)
    live = first + lax.broadcasted_iota(jnp.int32, (rows, 1), 0) < limit
    for head in range(group_size):
        columns = slice(head * HEAD_DIM, (head + 1) * HEAD_DIM)
        scores = lax.dot_general(
            query_ref[:, columns],
            key_ref[...],
            (((1,), (1,)), ((), ())),
            preferred_element_type=jnp.float32,
        ) * HEAD_DIM ** (-0.5)
        masked = jnp.where(allowed, scores, NEG_BIG)
        weights = jnp.exp(masked - jnp.max(masked, axis=1, keepdims=True))
        total = jnp.sum(weights, axis=1, keepdims=True)
        accum = jnp.dot(
            weights.astype(jnp.bfloat16), value_ref[...], preferred_element_type=jnp.float32
        )
        head_out = jnp.where(live, accum / jnp.where(live, total, 1.0), 0.0)
        out_ref[:, columns] = head_out.astype(jnp.bfloat16)


def attention(queries, key_value, limit, first):
    rows, count = queries.shape[0], key_value.shape[0]
    kv_local = key_value.shape[1] // (2 * HEAD_DIM)
    group_size = queries.shape[1] // (kv_local * HEAD_DIM)
    wide = (rows, group_size * HEAD_DIM)
    return pl.pallas_call(
        functools.partial(attention_kernel, group_size),
        grid=(kv_local,),
        out_shape=jax.ShapeDtypeStruct(queries.shape, jnp.bfloat16),
        in_specs=[
            pl.BlockSpec(memory_space=pltpu.SMEM),
            pl.BlockSpec(wide, lambda head: (0, head)),
            pl.BlockSpec((count, HEAD_DIM), lambda head: (0, head)),
            pl.BlockSpec((count, HEAD_DIM), lambda head: (0, head + kv_local)),
        ],
        out_specs=pl.BlockSpec(wide, lambda head: (0, head)),
        compiler_params=pltpu.CompilerParams(vmem_limit_bytes=40 * 1024 * 1024),
        cost_estimate=pl.CostEstimate(
            flops=4 * rows * count * queries.shape[1],
            bytes_accessed=4 * queries.size + 2 * key_value.size,
            transcendentals=rows * count * kv_local * group_size,
        ),
    )(jnp.stack([limit, first]), queries, key_value, key_value)


def body(
    length,
    residual,
    ssm_input,
    state_in,
    state_out,
    step_raw,
    decay_rate,
    ssm_gain,
    out_weight,
    norm_gain,
    query_weight,
    key_weight,
    value_weight,
):
    rows = residual.shape[0]
    local_heads = decay_rate.shape[0]
    head_width = ssm_input.shape[1] // local_heads
    seq_index = lax.axis_index("seq")
    limit = length[0]
    positions = seq_index * rows + jnp.arange(rows, dtype=jnp.int32)
    live_rows = positions < limit
    live = live_rows.astype(jnp.float32)
    delta = live[None, :] * jax.nn.softplus(step_raw)
    cumlog = jnp.cumsum(-decay_rate[:, None] * delta, axis=1)
    inputs = ssm_input.astype(jnp.float32).reshape(rows, local_heads, head_width)
    inner = jnp.dot(state_out, state_in.T, preferred_element_type=jnp.float32)
    causal = jnp.arange(rows)[:, None] >= jnp.arange(rows)[None, :]
    spread = cumlog[:, :, None] - cumlog[:, None, :]
    mixing = (
        jnp.where(causal[None], jnp.exp(jnp.where(causal[None], spread, 0.0)), 0.0)
        * inner[None]
        * delta[:, None, :]
    )
    within = jnp.einsum("hts,shp->thp", mixing, inputs, precision=HIGHEST)
    tail = jnp.exp(cumlog[:, -1:] - cumlog) * delta
    local_state = jnp.einsum(
        "hs,shp,sn->hpn", tail, inputs, state_in.astype(jnp.float32), precision=HIGHEST
    )
    incoming = incoming_state(cumlog[:, -1], local_state, "seq")
    carried = jnp.einsum("hpn,tn->thp", incoming, state_out.astype(jnp.float32), precision=HIGHEST)
    ssm_out = (within + jnp.exp(cumlog).T[:, :, None] * carried) * live[:, None, None]
    mean_square = jnp.mean(ssm_out * ssm_out, axis=2, keepdims=True)
    normed = (
        ssm_out * lax.rsqrt(mean_square + EPSILON) * ssm_gain.reshape(local_heads, head_width)
    ).astype(jnp.bfloat16)
    normed = normed.reshape(rows, local_heads * head_width)
    partial_value = jnp.dot(normed, out_weight, preferred_element_type=jnp.float32)
    layer_out, attn_in = line_sum_and_gather(
        partial_value, residual, norm_gain, lax.axis_size("head")
    )
    queries = jnp.dot(attn_in, query_weight, preferred_element_type=jnp.float32).astype(
        jnp.bfloat16
    )
    keys = jnp.dot(attn_in, key_weight, preferred_element_type=jnp.float32).astype(jnp.bfloat16)
    values = jnp.dot(attn_in, value_weight, preferred_element_type=jnp.float32).astype(jnp.bfloat16)
    key_value = lax.all_gather(
        jnp.concatenate([keys, values], axis=1), "seq", axis=0, tiled=True
    )
    head_out = attention(queries, key_value, limit, seq_index * rows)
    return (layer_out, head_out)


def solution(mesh):
    placed = (
        P("doc"),
        P(("doc", "seq"), "head"),
        P(("doc", "seq"), "head"),
        P(("doc", "seq"), None),
        P(("doc", "seq"), None),
        P(("doc", "head"), "seq"),
        P("head"),
        P("head"),
        P("head", None),
        P(),
        P(None, "head"),
        P(None, "head"),
        P(None, "head"),
    )
    return jax.shard_map(
        body,
        mesh=mesh,
        in_specs=placed,
        out_specs=(P(("doc", "seq"), "head"), P(("doc", "seq"), "head")),
        check_vma=False,
    )
```

```python
import functools

import jax
import jax.numpy as jnp
from jax import lax
from jax.experimental import pallas as pl
from jax.experimental.pallas import tpu as pltpu
from jax.sharding import PartitionSpec as P

HEAD_DIM = 128


EPSILON = 1e-05
NEG_BIG = -1e30
HIGHEST = lax.Precision.HIGHEST


def split_3(value):
    high = lax.reduce_precision(value, 8, 7)
    middle = lax.reduce_precision(value - high, 8, 7)
    low = value - high - middle
    return jnp.stack([high, middle, low], axis=1).astype(jnp.bfloat16)


def incoming_state(log_decay, local_state, axis):
    count, mine = (lax.axis_size(axis), lax.axis_index(axis))
    heads, width, states = local_state.shape
    decay_rows = jnp.pad(split_3(log_decay), ((0, 0), (0, states - 3)))
    packed = jnp.concatenate(
        [local_state.astype(jnp.bfloat16).reshape(heads * width, states), decay_rows], axis=0
    )
    pieces = lax.all_gather(packed, axis)
    logs = jnp.sum(pieces[:, heads * width :, :3].astype(jnp.float32), axis=2)
    order = jnp.arange(count)
    between = (order[None, :] > order[:, None]) & (order[None, :] < mine)
    reach = jnp.sum(jnp.where(between[:, :, None], logs[None], 0.0), axis=1)
    factor = jnp.where((order < mine)[:, None], jnp.exp(reach), 0.0)
    total = jnp.zeros(local_state.shape, jnp.float32)
    for position in range(count - 1):
        piece = pieces[position, : heads * width].reshape(heads, width, states)
        total += factor[position][:, None, None] * piece.astype(jnp.float32)
    return total


def line_kernel(
    count,
    shards,
    chunks,
    partial_ref,
    residual_ref,
    gain_ref,
    query_weight_ref,
    key_weight_ref,
    value_weight_ref,
    layer_ref,
    query_ref,
    key_value_ref,
    weight_ref,
    attn_ref,
    shared_ref,
    stage_ref,
    landed_ref,
    gathered_ref,
    total_ref,
    sum_send,
    sum_recv,
    copy_send,
    copy_recv,
    shard_send,
    shard_recv,
    weight_sem,
):
    mine = lax.axis_index("head")
    last = count - 1
    width = residual_ref.shape[1]
    rows = residual_ref.shape[0] // chunks
    place = (mine, last - mine)

    shard = lax.axis_index("seq")
    query_width = query_ref.shape[1]
    kv_width = key_weight_ref.shape[1]
    starts = (0, kv_width, 2 * kv_width)
    loads = [
        pltpu.make_async_copy(
            source, weight_ref.at[:, pl.ds(start, source.shape[1])], weight_sem.at[index]
        )
        for index, (source, start) in enumerate(
            zip((key_weight_ref, value_weight_ref, query_weight_ref), starts)
        )
    ]
    for load in loads:
        load.start()

    barrier = pltpu.get_barrier_semaphore()

    def greet(neighbour):
        pl.semaphore_signal(
            barrier, inc=1, device_id={"head": neighbour}, device_id_type=pl.DeviceIdType.MESH
        )

    @pl.when(mine > 0)
    def _():
        greet(mine - 1)

    @pl.when(mine < last)
    def _():
        greet(mine + 1)

    for offset in range(1, shards):
        other = (shard + offset) % shards
        pl.semaphore_signal(
            barrier, inc=1, device_id={"seq": other}, device_id_type=pl.DeviceIdType.MESH
        )

    @pl.when((mine == 0) | (mine == last))
    def _():
        pl.semaphore_wait(barrier, shards)

    @pl.when((mine > 0) & (mine < last))
    def _():
        pl.semaphore_wait(barrier, shards + 1)

    for other in range(shards):

        @pl.when(other > shard)
        def _():
            shared_ref[pl.ds(other * residual_ref.shape[0], residual_ref.shape[0])] = jnp.zeros(
                (residual_ref.shape[0], 2 * kv_width), jnp.bfloat16
            )

    def neighbour(way):
        return mine + 1 if way == 0 else mine - 1

    def real(way, position):
        return position if way == 0 else last - position

    def sum_copy(way, chunk, step):
        return pltpu.make_async_remote_copy(
            src_ref=stage_ref.at[way, chunk, step],
            dst_ref=landed_ref.at[way, chunk, step],
            send_sem=sum_send.at[way, chunk, step],
            recv_sem=sum_recv.at[way, chunk, step],
            device_id={"head": neighbour(way)},
            device_id_type=pl.DeviceIdType.MESH,
        )

    def block_copy(way, chunk, step, source):
        block = gathered_ref.at[source, pl.ds(chunk * rows, rows)]
        return pltpu.make_async_remote_copy(
            src_ref=block,
            dst_ref=block,
            send_sem=copy_send.at[way, chunk, step],
            recv_sem=copy_recv.at[way, chunk, step],
            device_id={"head": neighbour(way)},
            device_id_type=pl.DeviceIdType.MESH,
        )

    def shard_copy(chunk, offset, source):
        start = pl.multiple_of(source * residual_ref.shape[0] + chunk * rows, 16)
        block = shared_ref.at[pl.ds(start, rows)]
        return pltpu.make_async_remote_copy(
            src_ref=block,
            dst_ref=block,
            send_sem=shard_send.at[chunk, offset],
            recv_sem=shard_recv.at[chunk, offset],
            device_id={"seq": (shard + offset) % shards},
            device_id_type=pl.DeviceIdType.MESH,
        )

    def project(chunk):
        here = pl.ds(chunk * rows, rows)
        there = pl.ds(pl.multiple_of(shard * residual_ref.shape[0] + chunk * rows, 16), rows)

        def product(tile):
            columns = pl.ds(pl.multiple_of(tile * kv_width, 128), kv_width)
            return jnp.dot(
                attn_ref[here], weight_ref[:, columns], preferred_element_type=jnp.float32
            ).astype(jnp.bfloat16)

        if chunk == 0:
            for load in loads:
                load.wait()

        @pl.loop(0, 2)
        def _(tile):
            columns = pl.ds(pl.multiple_of(tile * kv_width, 128), kv_width)
            shared_ref[there, columns] = product(tile)

        for offset in range(1, shards):

            @pl.when(shard + offset < shards)
            def _():
                shard_copy(chunk, offset, shard).start()

        @pl.loop(0, query_width // kv_width)
        def _(tile):
            columns = pl.ds(pl.multiple_of(tile * kv_width, 128), kv_width)
            query_ref[here, columns] = product(tile + 2)

    def own_part(chunk, owner):
        columns = pl.ds(pl.multiple_of(owner * width, 128), width)
        return partial_ref[pl.ds(chunk * rows, rows), columns]

    def sum_step(chunk, step):
        for way in range(2):
            owner = real(way, last - step + place[way])

            @pl.when(place[way] == 0)
            def _():
                stage_ref[way, chunk, step] = own_part(chunk, owner).astype(jnp.bfloat16)
                sum_copy(way, chunk, step).start()

            if step == 0:
                continue

            @pl.when((place[way] <= step) & (place[way] > 0))
            def _():
                sum_copy(way, chunk, step - 1).wait_recv()
                arrived = landed_ref[way, chunk, step - 1].astype(jnp.float32)
                stage_ref[way, chunk, step] = (own_part(chunk, owner) + arrived).astype(
                    jnp.bfloat16
                )
                sum_copy(way, chunk, step).start()

    def finish_sum(chunk):
        here = pl.ds(chunk * rows, rows)
        total_ref[...] = residual_ref[here].astype(jnp.float32) + own_part(chunk, mine)
        for way in range(2):

            @pl.when(place[way] > 0)
            def _():
                sum_copy(way, chunk, last - 1).wait_recv()
                total_ref[...] += landed_ref[way, chunk, last - 1].astype(jnp.float32)

        layer_low = total_ref[...].astype(jnp.bfloat16)
        gathered_ref[mine, here] = layer_low
        layer_ref[here] = layer_low
        for way in range(2):

            @pl.when(place[way] < last)
            def _():
                block_copy(way, chunk, 0, mine).start()

    def forward(chunk, step):
        for way in range(2):
            source = real(way, place[way] - step)

            @pl.when(place[way] >= step)
            def _():
                block_copy(way, chunk, step - 1, source).wait_recv()

            @pl.when((place[way] >= step) & (place[way] < last))
            def _():
                block_copy(way, chunk, step, source).start()

    def normalise(chunk):
        for way in range(2):

            @pl.when(place[way] == last)
            def _():
                block_copy(way, chunk, last - 1, real(way, 0)).wait_recv()

        here = pl.ds(chunk * rows, rows)
        squares = jnp.zeros((rows, 1), jnp.float32)
        for source in range(count):
            block = gathered_ref[source, here].astype(jnp.float32)
            squares += jnp.sum(block * block, axis=1, keepdims=True)
        scale = lax.rsqrt(squares / (count * width) + EPSILON)
        for source in range(count):
            columns = slice(source * width, (source + 1) * width)
            block = gathered_ref[source, here].astype(jnp.float32)
            attn_ref[here, columns] = (block * scale * gain_ref[:, columns]).astype(jnp.bfloat16)

    for tick in range(chunks + 2 * last):
        for chunk in range(chunks):
            stage = tick - chunk
            if 0 <= stage < last:
                sum_step(chunk, stage)
            elif stage == last:
                finish_sum(chunk)
            elif last < stage < 2 * last:
                forward(chunk, stage - last)
        if 0 <= tick - 2 * last < chunks:
            normalise(tick - 2 * last)
            project(tick - 2 * last)

    for chunk in range(chunks):
        for step in range(last):
            for way in range(2):

                @pl.when(place[way] <= step)
                def _():
                    sum_copy(way, chunk, step).wait_send()

                @pl.when((place[way] >= step) & (place[way] < last))
                def _():
                    block_copy(way, chunk, step, real(way, place[way] - step)).wait_send()

        for offset in range(1, shards):

            @pl.when(shard + offset < shards)
            def _():
                shard_copy(chunk, offset, shard).wait_send()

            @pl.when(shard >= offset)
            def _():
                shard_copy(chunk, offset, shard - offset).wait_recv()

    key_value_ref[...] = shared_ref[...]


def line_layer(partial_value, residual, norm_gain, weights, count, shards):
    rows, width = residual.shape
    model_width = width * count
    query_width, kv_width = weights[0].shape[1], weights[1].shape[1]
    chunks = 4 if rows % 64 == 0 else 1
    piece = rows // chunks
    messages = (2, chunks, count - 1)
    vmem = pl.BlockSpec(memory_space=pltpu.VMEM)
    return pl.pallas_call(
        functools.partial(line_kernel, count, shards, chunks),
        out_shape=(
            jax.ShapeDtypeStruct((rows, width), jnp.bfloat16),
            jax.ShapeDtypeStruct((rows, query_width), jnp.bfloat16),
            jax.ShapeDtypeStruct((shards * rows, 2 * kv_width), jnp.bfloat16),
        ),
        in_specs=[vmem] * 3 + [pl.BlockSpec(memory_space=pltpu.HBM)] * 3,
        out_specs=[vmem] * 3,
        scratch_shapes=[
            pltpu.VMEM((model_width, 2 * kv_width + query_width), jnp.bfloat16),
            pltpu.VMEM((rows, model_width), jnp.bfloat16),
            pltpu.VMEM((shards * rows, 2 * kv_width), jnp.bfloat16),
            pltpu.VMEM(messages + (piece, width), jnp.bfloat16),
            pltpu.VMEM(messages + (piece, width), jnp.bfloat16),
            pltpu.VMEM((count, rows, width), jnp.bfloat16),
            pltpu.VMEM((piece, width), jnp.float32),
            pltpu.SemaphoreType.DMA(messages),
            pltpu.SemaphoreType.DMA(messages),
            pltpu.SemaphoreType.DMA(messages),
            pltpu.SemaphoreType.DMA(messages),
            pltpu.SemaphoreType.DMA((chunks, shards)),
            pltpu.SemaphoreType.DMA((chunks, shards)),
            pltpu.SemaphoreType.DMA((3,)),
        ],
        compiler_params=pltpu.CompilerParams(
            collective_id=0, has_side_effects=True, vmem_limit_bytes=52 * 1024 * 1024
        ),
    )(partial_value, residual, norm_gain.reshape(1, model_width), *weights)


def attention_kernel(group_size, limits_ref, query_ref, key_ref, value_ref, out_ref):
    rows, count = query_ref.shape[0], key_ref.shape[0]
    limit, first = limits_ref[0], limits_ref[1]
    key_pos = lax.broadcasted_iota(jnp.int32, (rows, count), 1)
    positions = first + lax.broadcasted_iota(jnp.int32, (rows, count), 0)
    allowed = (key_pos <= positions) & (key_pos < limit)
    live = first + lax.broadcasted_iota(jnp.int32, (rows, 1), 0) < limit
    for head in range(group_size):
        columns = slice(head * HEAD_DIM, (head + 1) * HEAD_DIM)
        scores = lax.dot_general(
            query_ref[:, columns],
            key_ref[...],
            (((1,), (1,)), ((), ())),
            preferred_element_type=jnp.float32,
        ) * HEAD_DIM ** (-0.5)
        masked = jnp.where(allowed, scores, NEG_BIG)
        weights = jnp.exp(masked - jnp.max(masked, axis=1, keepdims=True))
        total = jnp.sum(weights, axis=1, keepdims=True)
        accum = jnp.dot(
            weights.astype(jnp.bfloat16), value_ref[...], preferred_element_type=jnp.float32
        )
        head_out = jnp.where(live, accum / jnp.where(live, total, 1.0), 0.0)
        out_ref[:, columns] = head_out.astype(jnp.bfloat16)


def attention(queries, key_value, limit, first):
    rows, count = queries.shape[0], key_value.shape[0]
    kv_local = key_value.shape[1] // (2 * HEAD_DIM)
    group_size = queries.shape[1] // (kv_local * HEAD_DIM)
    wide = (rows, group_size * HEAD_DIM)
    return pl.pallas_call(
        functools.partial(attention_kernel, group_size),
        grid=(kv_local,),
        out_shape=jax.ShapeDtypeStruct(queries.shape, jnp.bfloat16),
        in_specs=[
            pl.BlockSpec(memory_space=pltpu.SMEM),
            pl.BlockSpec(wide, lambda head: (0, head)),
            pl.BlockSpec((count, HEAD_DIM), lambda head: (0, head)),
            pl.BlockSpec((count, HEAD_DIM), lambda head: (0, head + kv_local)),
        ],
        out_specs=pl.BlockSpec(wide, lambda head: (0, head)),
        compiler_params=pltpu.CompilerParams(vmem_limit_bytes=40 * 1024 * 1024),
        cost_estimate=pl.CostEstimate(
            flops=4 * rows * count * queries.shape[1],
            bytes_accessed=4 * queries.size + 2 * key_value.size,
            transcendentals=rows * count * kv_local * group_size,
        ),
    )(jnp.stack([limit, first]), queries, key_value, key_value)


def body(
    length,
    residual,
    ssm_input,
    state_in,
    state_out,
    step_raw,
    decay_rate,
    ssm_gain,
    out_weight,
    norm_gain,
    query_weight,
    key_weight,
    value_weight,
):
    rows = residual.shape[0]
    local_heads = decay_rate.shape[0]
    head_width = ssm_input.shape[1] // local_heads
    seq_index = lax.axis_index("seq")
    limit = length[0]
    positions = seq_index * rows + jnp.arange(rows, dtype=jnp.int32)
    live_rows = positions < limit
    live = live_rows.astype(jnp.float32)
    delta = live[None, :] * jax.nn.softplus(step_raw)
    cumlog = jnp.cumsum(-decay_rate[:, None] * delta, axis=1)
    inputs = ssm_input.astype(jnp.float32).reshape(rows, local_heads, head_width)
    inner = jnp.dot(state_out, state_in.T, preferred_element_type=jnp.float32)
    causal = jnp.arange(rows)[:, None] >= jnp.arange(rows)[None, :]
    spread = cumlog[:, :, None] - cumlog[:, None, :]
    mixing = (
        jnp.where(causal[None], jnp.exp(jnp.where(causal[None], spread, 0.0)), 0.0)
        * inner[None]
        * delta[:, None, :]
    )
    within = jnp.einsum("hts,shp->thp", mixing, inputs, precision=HIGHEST)
    tail = jnp.exp(cumlog[:, -1:] - cumlog) * delta
    local_state = jnp.einsum(
        "hs,shp,sn->hpn", tail, inputs, state_in.astype(jnp.float32), precision=HIGHEST
    )
    incoming = incoming_state(cumlog[:, -1], local_state, "seq")
    carried = jnp.einsum("hpn,tn->thp", incoming, state_out.astype(jnp.float32), precision=HIGHEST)
    ssm_out = (within + jnp.exp(cumlog).T[:, :, None] * carried) * live[:, None, None]
    mean_square = jnp.mean(ssm_out * ssm_out, axis=2, keepdims=True)
    normed = (
        ssm_out * lax.rsqrt(mean_square + EPSILON) * ssm_gain.reshape(local_heads, head_width)
    ).astype(jnp.bfloat16)
    normed = normed.reshape(rows, local_heads * head_width)
    partial_value = jnp.dot(normed, out_weight, preferred_element_type=jnp.float32)
    layer_out, queries, key_value = line_layer(
        partial_value,
        residual,
        norm_gain,
        (query_weight, key_weight, value_weight),
        lax.axis_size("head"),
        lax.axis_size("seq"),
    )
    head_out = attention(queries, key_value, limit, seq_index * rows)
    return (layer_out, head_out)


def solution(mesh):
    placed = (
        P("doc"),
        P(("doc", "seq"), "head"),
        P(("doc", "seq"), "head"),
        P(("doc", "seq"), None),
        P(("doc", "seq"), None),
        P(("doc", "head"), "seq"),
        P("head"),
        P("head"),
        P("head", None),
        P(),
        P(None, "head"),
        P(None, "head"),
        P(None, "head"),
    )
    return jax.shard_map(
        body,
        mesh=mesh,
        in_specs=placed,
        out_specs=(P(("doc", "seq"), "head"), P(("doc", "seq"), "head")),
        check_vma=False,
    )
```

```python
import functools

import jax
import jax.numpy as jnp
from jax import lax
from jax.experimental import pallas as pl
from jax.experimental.pallas import tpu as pltpu
from jax.sharding import PartitionSpec as P

HEAD_DIM = 128


EPSILON = 1e-05
NEG_BIG = -1e30
HIGHEST = lax.Precision.HIGHEST


def chain_kernel(
    count, chunks, decay_ref, state_ref, incoming_ref, stage_ref, landed_ref, send_sem, recv_sem
):
    mine = lax.axis_index("seq")
    last = count - 1
    heads = state_ref.shape[0] // chunks
    barrier = pltpu.get_barrier_semaphore()

    def greet(neighbour):
        pl.semaphore_signal(
            barrier, inc=1, device_id={"seq": neighbour}, device_id_type=pl.DeviceIdType.MESH
        )

    @pl.when(mine > 0)
    def _():
        greet(mine - 1)

    @pl.when(mine < last)
    def _():
        greet(mine + 1)

    @pl.when((mine == 0) | (mine == last))
    def _():
        pl.semaphore_wait(barrier, 1)

    @pl.when((mine > 0) & (mine < last))
    def _():
        pl.semaphore_wait(barrier, 2)

    def copy(chunk):
        return pltpu.make_async_remote_copy(
            src_ref=stage_ref.at[chunk],
            dst_ref=landed_ref.at[chunk],
            send_sem=send_sem.at[chunk],
            recv_sem=recv_sem.at[chunk],
            device_id={"seq": mine + 1},
            device_id_type=pl.DeviceIdType.MESH,
        )

    for chunk in range(chunks):
        here = pl.ds(chunk * heads, heads)

        @pl.when(mine == 0)
        def _():
            incoming_ref[here] = jnp.zeros((heads,) + state_ref.shape[1:], jnp.float32)

        @pl.when(mine > 0)
        def _():
            copy(chunk).wait_recv()
            incoming_ref[here] = landed_ref[chunk].astype(jnp.float32)

        @pl.when(mine < last)
        def _():
            for index in range(heads):
                head = chunk * heads + index
                outgoing = decay_ref[head] * incoming_ref[head] + state_ref[head]
                stage_ref[chunk, index] = outgoing.astype(jnp.bfloat16)
            copy(chunk).start()

    for chunk in range(chunks):

        @pl.when(mine < last)
        def _():
            copy(chunk).wait_send()


def incoming_state(block_decay, local_state, count):
    heads, width, states = local_state.shape
    chunks = 4 if heads % 4 == 0 else 1
    slots = (chunks, heads // chunks, width, states)
    return pl.pallas_call(
        functools.partial(chain_kernel, count, chunks),
        out_shape=jax.ShapeDtypeStruct(local_state.shape, jnp.float32),
        in_specs=[
            pl.BlockSpec(memory_space=pltpu.SMEM),
            pl.BlockSpec(memory_space=pltpu.VMEM),
        ],
        out_specs=pl.BlockSpec(memory_space=pltpu.VMEM),
        scratch_shapes=[
            pltpu.VMEM(slots, jnp.bfloat16),
            pltpu.VMEM(slots, jnp.bfloat16),
            pltpu.SemaphoreType.DMA((chunks,)),
            pltpu.SemaphoreType.DMA((chunks,)),
        ],
        compiler_params=pltpu.CompilerParams(collective_id=1, has_side_effects=True),
    )(block_decay, local_state)


def line_kernel(
    count,
    shards,
    chunks,
    partial_ref,
    residual_ref,
    gain_ref,
    query_weight_ref,
    key_weight_ref,
    value_weight_ref,
    layer_ref,
    query_ref,
    key_value_ref,
    weight_ref,
    attn_ref,
    shared_ref,
    stage_ref,
    landed_ref,
    gathered_ref,
    total_ref,
    sum_send,
    sum_recv,
    copy_send,
    copy_recv,
    shard_send,
    shard_recv,
    weight_sem,
):
    mine = lax.axis_index("head")
    last = count - 1
    width = residual_ref.shape[1]
    rows = residual_ref.shape[0] // chunks
    place = (mine, last - mine)

    shard = lax.axis_index("seq")
    query_width = query_ref.shape[1]
    kv_width = key_weight_ref.shape[1]
    starts = (0, kv_width, 2 * kv_width)
    loads = [
        pltpu.make_async_copy(
            source, weight_ref.at[:, pl.ds(start, source.shape[1])], weight_sem.at[index]
        )
        for index, (source, start) in enumerate(
            zip((key_weight_ref, value_weight_ref, query_weight_ref), starts)
        )
    ]
    for load in loads:
        load.start()

    barrier = pltpu.get_barrier_semaphore()

    def greet(neighbour):
        pl.semaphore_signal(
            barrier, inc=1, device_id={"head": neighbour}, device_id_type=pl.DeviceIdType.MESH
        )

    @pl.when(mine > 0)
    def _():
        greet(mine - 1)

    @pl.when(mine < last)
    def _():
        greet(mine + 1)

    for offset in range(1, shards):
        other = (shard + offset) % shards
        pl.semaphore_signal(
            barrier, inc=1, device_id={"seq": other}, device_id_type=pl.DeviceIdType.MESH
        )

    @pl.when((mine == 0) | (mine == last))
    def _():
        pl.semaphore_wait(barrier, shards)

    @pl.when((mine > 0) & (mine < last))
    def _():
        pl.semaphore_wait(barrier, shards + 1)

    for other in range(shards):

        @pl.when(other > shard)
        def _():
            shared_ref[pl.ds(other * residual_ref.shape[0], residual_ref.shape[0])] = jnp.zeros(
                (residual_ref.shape[0], 2 * kv_width), jnp.bfloat16
            )

    def neighbour(way):
        return mine + 1 if way == 0 else mine - 1

    def real(way, position):
        return position if way == 0 else last - position

    def sum_copy(way, chunk, step):
        return pltpu.make_async_remote_copy(
            src_ref=stage_ref.at[way, chunk, step],
            dst_ref=landed_ref.at[way, chunk, step],
            send_sem=sum_send.at[way, chunk, step],
            recv_sem=sum_recv.at[way, chunk, step],
            device_id={"head": neighbour(way)},
            device_id_type=pl.DeviceIdType.MESH,
        )

    def block_copy(way, chunk, step, source):
        block = gathered_ref.at[source, pl.ds(chunk * rows, rows)]
        return pltpu.make_async_remote_copy(
            src_ref=block,
            dst_ref=block,
            send_sem=copy_send.at[way, chunk, step],
            recv_sem=copy_recv.at[way, chunk, step],
            device_id={"head": neighbour(way)},
            device_id_type=pl.DeviceIdType.MESH,
        )

    def shard_copy(chunk, offset, source):
        start = pl.multiple_of(source * residual_ref.shape[0] + chunk * rows, 16)
        block = shared_ref.at[pl.ds(start, rows)]
        return pltpu.make_async_remote_copy(
            src_ref=block,
            dst_ref=block,
            send_sem=shard_send.at[chunk, offset],
            recv_sem=shard_recv.at[chunk, offset],
            device_id={"seq": (shard + offset) % shards},
            device_id_type=pl.DeviceIdType.MESH,
        )

    def project(chunk):
        here = pl.ds(chunk * rows, rows)
        there = pl.ds(pl.multiple_of(shard * residual_ref.shape[0] + chunk * rows, 16), rows)

        def product(tile):
            columns = pl.ds(pl.multiple_of(tile * kv_width, 128), kv_width)
            return jnp.dot(
                attn_ref[here], weight_ref[:, columns], preferred_element_type=jnp.float32
            ).astype(jnp.bfloat16)

        if chunk == 0:
            for load in loads:
                load.wait()

        @pl.loop(0, 2)
        def _(tile):
            columns = pl.ds(pl.multiple_of(tile * kv_width, 128), kv_width)
            shared_ref[there, columns] = product(tile)

        for offset in range(1, shards):

            @pl.when(shard + offset < shards)
            def _():
                shard_copy(chunk, offset, shard).start()

        @pl.loop(0, query_width // kv_width)
        def _(tile):
            columns = pl.ds(pl.multiple_of(tile * kv_width, 128), kv_width)
            query_ref[here, columns] = product(tile + 2)

    def own_part(chunk, owner):
        columns = pl.ds(pl.multiple_of(owner * width, 128), width)
        return partial_ref[pl.ds(chunk * rows, rows), columns]

    def sum_step(chunk, step):
        for way in range(2):
            owner = real(way, last - step + place[way])

            @pl.when(place[way] == 0)
            def _():
                stage_ref[way, chunk, step] = own_part(chunk, owner).astype(jnp.bfloat16)
                sum_copy(way, chunk, step).start()

            if step == 0:
                continue

            @pl.when((place[way] <= step) & (place[way] > 0))
            def _():
                sum_copy(way, chunk, step - 1).wait_recv()
                arrived = landed_ref[way, chunk, step - 1].astype(jnp.float32)
                stage_ref[way, chunk, step] = (own_part(chunk, owner) + arrived).astype(
                    jnp.bfloat16
                )
                sum_copy(way, chunk, step).start()

    def finish_sum(chunk):
        here = pl.ds(chunk * rows, rows)
        total_ref[...] = residual_ref[here].astype(jnp.float32) + own_part(chunk, mine)
        for way in range(2):

            @pl.when(place[way] > 0)
            def _():
                sum_copy(way, chunk, last - 1).wait_recv()
                total_ref[...] += landed_ref[way, chunk, last - 1].astype(jnp.float32)

        layer_low = total_ref[...].astype(jnp.bfloat16)
        gathered_ref[mine, here] = layer_low
        layer_ref[here] = layer_low
        for way in range(2):

            @pl.when(place[way] < last)
            def _():
                block_copy(way, chunk, 0, mine).start()

    def forward(chunk, step):
        for way in range(2):
            source = real(way, place[way] - step)

            @pl.when(place[way] >= step)
            def _():
                block_copy(way, chunk, step - 1, source).wait_recv()

            @pl.when((place[way] >= step) & (place[way] < last))
            def _():
                block_copy(way, chunk, step, source).start()

    def normalise(chunk):
        for way in range(2):

            @pl.when(place[way] == last)
            def _():
                block_copy(way, chunk, last - 1, real(way, 0)).wait_recv()

        here = pl.ds(chunk * rows, rows)
        squares = jnp.zeros((rows, 1), jnp.float32)
        for source in range(count):
            block = gathered_ref[source, here].astype(jnp.float32)
            squares += jnp.sum(block * block, axis=1, keepdims=True)
        scale = lax.rsqrt(squares / (count * width) + EPSILON)
        for source in range(count):
            columns = slice(source * width, (source + 1) * width)
            block = gathered_ref[source, here].astype(jnp.float32)
            attn_ref[here, columns] = (block * scale * gain_ref[:, columns]).astype(jnp.bfloat16)

    for tick in range(chunks + 2 * last):
        for chunk in range(chunks):
            stage = tick - chunk
            if 0 <= stage < last:
                sum_step(chunk, stage)
            elif stage == last:
                finish_sum(chunk)
            elif last < stage < 2 * last:
                forward(chunk, stage - last)
        if 0 <= tick - 2 * last < chunks:
            normalise(tick - 2 * last)
            project(tick - 2 * last)

    for chunk in range(chunks):
        for step in range(last):
            for way in range(2):

                @pl.when(place[way] <= step)
                def _():
                    sum_copy(way, chunk, step).wait_send()

                @pl.when((place[way] >= step) & (place[way] < last))
                def _():
                    block_copy(way, chunk, step, real(way, place[way] - step)).wait_send()

        for offset in range(1, shards):

            @pl.when(shard + offset < shards)
            def _():
                shard_copy(chunk, offset, shard).wait_send()

            @pl.when(shard >= offset)
            def _():
                shard_copy(chunk, offset, shard - offset).wait_recv()

    key_value_ref[...] = shared_ref[...]


def line_layer(partial_value, residual, norm_gain, weights, count, shards):
    rows, width = residual.shape
    model_width = width * count
    query_width, kv_width = weights[0].shape[1], weights[1].shape[1]
    chunks = 4 if rows % 64 == 0 else 1
    piece = rows // chunks
    messages = (2, chunks, count - 1)
    vmem = pl.BlockSpec(memory_space=pltpu.VMEM)
    return pl.pallas_call(
        functools.partial(line_kernel, count, shards, chunks),
        out_shape=(
            jax.ShapeDtypeStruct((rows, width), jnp.bfloat16),
            jax.ShapeDtypeStruct((rows, query_width), jnp.bfloat16),
            jax.ShapeDtypeStruct((shards * rows, 2 * kv_width), jnp.bfloat16),
        ),
        in_specs=[vmem] * 3 + [pl.BlockSpec(memory_space=pltpu.HBM)] * 3,
        out_specs=[vmem] * 3,
        scratch_shapes=[
            pltpu.VMEM((model_width, 2 * kv_width + query_width), jnp.bfloat16),
            pltpu.VMEM((rows, model_width), jnp.bfloat16),
            pltpu.VMEM((shards * rows, 2 * kv_width), jnp.bfloat16),
            pltpu.VMEM(messages + (piece, width), jnp.bfloat16),
            pltpu.VMEM(messages + (piece, width), jnp.bfloat16),
            pltpu.VMEM((count, rows, width), jnp.bfloat16),
            pltpu.VMEM((piece, width), jnp.float32),
            pltpu.SemaphoreType.DMA(messages),
            pltpu.SemaphoreType.DMA(messages),
            pltpu.SemaphoreType.DMA(messages),
            pltpu.SemaphoreType.DMA(messages),
            pltpu.SemaphoreType.DMA((chunks, shards)),
            pltpu.SemaphoreType.DMA((chunks, shards)),
            pltpu.SemaphoreType.DMA((3,)),
        ],
        compiler_params=pltpu.CompilerParams(
            collective_id=0, has_side_effects=True, vmem_limit_bytes=52 * 1024 * 1024
        ),
    )(partial_value, residual, norm_gain.reshape(1, model_width), *weights)


def attention_kernel(group_size, limits_ref, query_ref, key_ref, value_ref, out_ref):
    rows, count = query_ref.shape[0], key_ref.shape[0]
    limit, first = limits_ref[0], limits_ref[1]
    key_pos = lax.broadcasted_iota(jnp.int32, (rows, count), 1)
    positions = first + lax.broadcasted_iota(jnp.int32, (rows, count), 0)
    allowed = (key_pos <= positions) & (key_pos < limit)
    live = first + lax.broadcasted_iota(jnp.int32, (rows, 1), 0) < limit
    for head in range(group_size):
        columns = slice(head * HEAD_DIM, (head + 1) * HEAD_DIM)
        scores = lax.dot_general(
            query_ref[:, columns],
            key_ref[...],
            (((1,), (1,)), ((), ())),
            preferred_element_type=jnp.float32,
        ) * HEAD_DIM ** (-0.5)
        masked = jnp.where(allowed, scores, NEG_BIG)
        weights = jnp.exp(masked - jnp.max(masked, axis=1, keepdims=True))
        total = jnp.sum(weights, axis=1, keepdims=True)
        accum = jnp.dot(
            weights.astype(jnp.bfloat16), value_ref[...], preferred_element_type=jnp.float32
        )
        head_out = jnp.where(live, accum / jnp.where(live, total, 1.0), 0.0)
        out_ref[:, columns] = head_out.astype(jnp.bfloat16)


def attention(queries, key_value, limit, first):
    rows, count = queries.shape[0], key_value.shape[0]
    kv_local = key_value.shape[1] // (2 * HEAD_DIM)
    group_size = queries.shape[1] // (kv_local * HEAD_DIM)
    wide = (rows, group_size * HEAD_DIM)
    return pl.pallas_call(
        functools.partial(attention_kernel, group_size),
        grid=(kv_local,),
        out_shape=jax.ShapeDtypeStruct(queries.shape, jnp.bfloat16),
        in_specs=[
            pl.BlockSpec(memory_space=pltpu.SMEM),
            pl.BlockSpec(wide, lambda head: (0, head)),
            pl.BlockSpec((count, HEAD_DIM), lambda head: (0, head)),
            pl.BlockSpec((count, HEAD_DIM), lambda head: (0, head + kv_local)),
        ],
        out_specs=pl.BlockSpec(wide, lambda head: (0, head)),
        compiler_params=pltpu.CompilerParams(vmem_limit_bytes=40 * 1024 * 1024),
        cost_estimate=pl.CostEstimate(
            flops=4 * rows * count * queries.shape[1],
            bytes_accessed=4 * queries.size + 2 * key_value.size,
            transcendentals=rows * count * kv_local * group_size,
        ),
    )(jnp.stack([limit, first]), queries, key_value, key_value)


def body(
    length,
    residual,
    ssm_input,
    state_in,
    state_out,
    step_raw,
    decay_rate,
    ssm_gain,
    out_weight,
    norm_gain,
    query_weight,
    key_weight,
    value_weight,
):
    rows = residual.shape[0]
    local_heads = decay_rate.shape[0]
    head_width = ssm_input.shape[1] // local_heads
    seq_index = lax.axis_index("seq")
    limit = length[0]
    positions = seq_index * rows + jnp.arange(rows, dtype=jnp.int32)
    live_rows = positions < limit
    live = live_rows.astype(jnp.float32)
    delta = live[None, :] * jax.nn.softplus(step_raw)
    cumlog = jnp.cumsum(-decay_rate[:, None] * delta, axis=1)
    inputs = ssm_input.astype(jnp.float32).reshape(rows, local_heads, head_width)
    inner = jnp.dot(state_out, state_in.T, preferred_element_type=jnp.float32)
    causal = jnp.arange(rows)[:, None] >= jnp.arange(rows)[None, :]
    spread = cumlog[:, :, None] - cumlog[:, None, :]
    mixing = (
        jnp.where(causal[None], jnp.exp(jnp.where(causal[None], spread, 0.0)), 0.0)
        * inner[None]
        * delta[:, None, :]
    )
    within = jnp.einsum("hts,shp->thp", mixing, inputs, precision=HIGHEST)
    tail = jnp.exp(cumlog[:, -1:] - cumlog) * delta
    local_state = jnp.einsum(
        "hs,shp,sn->hpn", tail, inputs, state_in.astype(jnp.float32), precision=HIGHEST
    )
    incoming = incoming_state(jnp.exp(cumlog[:, -1]), local_state, lax.axis_size("seq"))
    carried = jnp.einsum("hpn,tn->thp", incoming, state_out.astype(jnp.float32), precision=HIGHEST)
    ssm_out = (within + jnp.exp(cumlog).T[:, :, None] * carried) * live[:, None, None]
    mean_square = jnp.mean(ssm_out * ssm_out, axis=2, keepdims=True)
    normed = (
        ssm_out * lax.rsqrt(mean_square + EPSILON) * ssm_gain.reshape(local_heads, head_width)
    ).astype(jnp.bfloat16)
    normed = normed.reshape(rows, local_heads * head_width)
    partial_value = jnp.dot(normed, out_weight, preferred_element_type=jnp.float32)
    layer_out, queries, key_value = line_layer(
        partial_value,
        residual,
        norm_gain,
        (query_weight, key_weight, value_weight),
        lax.axis_size("head"),
        lax.axis_size("seq"),
    )
    head_out = attention(queries, key_value, limit, seq_index * rows)
    return (layer_out, head_out)


def solution(mesh):
    placed = (
        P("doc"),
        P(("doc", "seq"), "head"),
        P(("doc", "seq"), "head"),
        P(("doc", "seq"), None),
        P(("doc", "seq"), None),
        P(("doc", "head"), "seq"),
        P("head"),
        P("head"),
        P("head", None),
        P(),
        P(None, "head"),
        P(None, "head"),
        P(None, "head"),
    )
    return jax.shard_map(
        body,
        mesh=mesh,
        in_specs=placed,
        out_specs=(P(("doc", "seq"), "head"), P(("doc", "seq"), "head")),
        check_vma=False,
    )
```

```python
import functools

import jax
import jax.numpy as jnp
from jax import lax
from jax.experimental import pallas as pl
from jax.experimental.pallas import tpu as pltpu
from jax.sharding import PartitionSpec as P

HEAD_DIM = 128


EPSILON = 1e-05
NEG_BIG = -1e30
HIGHEST = lax.Precision.HIGHEST


def chain_kernel(
    count, chunks, decay_ref, state_ref, incoming_ref, stage_ref, landed_ref, send_sem, recv_sem
):
    mine = lax.axis_index("seq")
    last = count - 1
    heads = state_ref.shape[0] // chunks
    barrier = pltpu.get_barrier_semaphore()

    def greet(neighbour):
        pl.semaphore_signal(
            barrier, inc=1, device_id={"seq": neighbour}, device_id_type=pl.DeviceIdType.MESH
        )

    @pl.when(mine > 0)
    def _():
        greet(mine - 1)

    @pl.when(mine < last)
    def _():
        greet(mine + 1)

    @pl.when((mine == 0) | (mine == last))
    def _():
        pl.semaphore_wait(barrier, 1)

    @pl.when((mine > 0) & (mine < last))
    def _():
        pl.semaphore_wait(barrier, 2)

    def copy(chunk):
        return pltpu.make_async_remote_copy(
            src_ref=stage_ref.at[chunk],
            dst_ref=landed_ref.at[chunk],
            send_sem=send_sem.at[chunk],
            recv_sem=recv_sem.at[chunk],
            device_id={"seq": mine + 1},
            device_id_type=pl.DeviceIdType.MESH,
        )

    for chunk in range(chunks):
        here = pl.ds(chunk * heads, heads)

        @pl.when(mine == 0)
        def _():
            incoming_ref[here] = jnp.zeros((heads,) + state_ref.shape[1:], jnp.float32)

        @pl.when(mine > 0)
        def _():
            copy(chunk).wait_recv()
            incoming_ref[here] = landed_ref[chunk].astype(jnp.float32)

        @pl.when(mine < last)
        def _():
            for index in range(heads):
                head = chunk * heads + index
                outgoing = decay_ref[head] * incoming_ref[head] + state_ref[head]
                stage_ref[chunk, index] = outgoing.astype(jnp.bfloat16)
            copy(chunk).start()

    for chunk in range(chunks):

        @pl.when(mine < last)
        def _():
            copy(chunk).wait_send()


def incoming_state(block_decay, local_state, count):
    heads, width, states = local_state.shape
    chunks = 4 if heads % 4 == 0 else 1
    slots = (chunks, heads // chunks, width, states)
    return pl.pallas_call(
        functools.partial(chain_kernel, count, chunks),
        out_shape=jax.ShapeDtypeStruct(local_state.shape, jnp.float32),
        in_specs=[
            pl.BlockSpec(memory_space=pltpu.SMEM),
            pl.BlockSpec(memory_space=pltpu.VMEM),
        ],
        out_specs=pl.BlockSpec(memory_space=pltpu.VMEM),
        scratch_shapes=[
            pltpu.VMEM(slots, jnp.bfloat16),
            pltpu.VMEM(slots, jnp.bfloat16),
            pltpu.SemaphoreType.DMA((chunks,)),
            pltpu.SemaphoreType.DMA((chunks,)),
        ],
        compiler_params=pltpu.CompilerParams(collective_id=1, has_side_effects=True),
    )(block_decay, local_state)


def line_kernel(
    count,
    shards,
    chunks,
    normed_ref,
    out_weight_ref,
    residual_ref,
    gain_ref,
    query_weight_ref,
    key_weight_ref,
    value_weight_ref,
    layer_ref,
    query_ref,
    key_value_ref,
    block_weight_ref,
    partial_ref,
    weight_ref,
    attn_ref,
    shared_ref,
    stage_ref,
    landed_ref,
    gathered_ref,
    total_ref,
    sum_send,
    sum_recv,
    copy_send,
    copy_recv,
    shard_send,
    shard_recv,
    weight_sem,
    block_sem,
):
    mine = lax.axis_index("head")
    last = count - 1
    width = residual_ref.shape[1]
    rows = residual_ref.shape[0] // chunks
    place = (mine, last - mine)

    shard = lax.axis_index("seq")
    query_width = query_ref.shape[1]
    kv_width = key_weight_ref.shape[1]
    starts = (0, kv_width, 2 * kv_width)
    loads = [
        pltpu.make_async_copy(
            source, weight_ref.at[:, pl.ds(start, source.shape[1])], weight_sem.at[index]
        )
        for index, (source, start) in enumerate(
            zip((key_weight_ref, value_weight_ref, query_weight_ref), starts)
        )
    ]

    def ordered(index):
        return jnp.where(2 * mine < count, last - index, index)

    def block_load(index):
        columns = pl.ds(pl.multiple_of(ordered(index) * width, 128), width)
        return pltpu.make_async_copy(
            out_weight_ref.at[:, columns], block_weight_ref.at[index], block_sem.at[index]
        )

    for index in range(count):
        block_load(index).start()
    for load in loads:
        load.start()

    def compute_block(index):
        block_load(index).wait()
        tile = min(width, 256)

        @pl.loop(0, width // tile)
        def _(step):
            columns = pl.ds(pl.multiple_of(step * tile, 128), tile)
            partial_ref[ordered(index), :, columns] = jnp.dot(
                normed_ref[...],
                block_weight_ref[index, :, columns],
                preferred_element_type=jnp.float32,
            )

    barrier = pltpu.get_barrier_semaphore()

    def greet(neighbour):
        pl.semaphore_signal(
            barrier, inc=1, device_id={"head": neighbour}, device_id_type=pl.DeviceIdType.MESH
        )

    @pl.when(mine > 0)
    def _():
        greet(mine - 1)

    @pl.when(mine < last)
    def _():
        greet(mine + 1)

    for offset in range(1, shards):
        other = (shard + offset) % shards
        pl.semaphore_signal(
            barrier, inc=1, device_id={"seq": other}, device_id_type=pl.DeviceIdType.MESH
        )

    @pl.when((mine == 0) | (mine == last))
    def _():
        pl.semaphore_wait(barrier, shards)

    @pl.when((mine > 0) & (mine < last))
    def _():
        pl.semaphore_wait(barrier, shards + 1)

    for other in range(shards):

        @pl.when(other > shard)
        def _():
            shared_ref[pl.ds(other * residual_ref.shape[0], residual_ref.shape[0])] = jnp.zeros(
                (residual_ref.shape[0], 2 * kv_width), jnp.bfloat16
            )

    def neighbour(way):
        return mine + 1 if way == 0 else mine - 1

    def real(way, position):
        return position if way == 0 else last - position

    def sum_copy(way, chunk, step):
        return pltpu.make_async_remote_copy(
            src_ref=stage_ref.at[way, chunk, step],
            dst_ref=landed_ref.at[way, chunk, step],
            send_sem=sum_send.at[way, chunk, step],
            recv_sem=sum_recv.at[way, chunk, step],
            device_id={"head": neighbour(way)},
            device_id_type=pl.DeviceIdType.MESH,
        )

    def block_copy(way, chunk, step, source):
        block = gathered_ref.at[source, pl.ds(chunk * rows, rows)]
        return pltpu.make_async_remote_copy(
            src_ref=block,
            dst_ref=block,
            send_sem=copy_send.at[way, chunk, step],
            recv_sem=copy_recv.at[way, chunk, step],
            device_id={"head": neighbour(way)},
            device_id_type=pl.DeviceIdType.MESH,
        )

    def shard_copy(chunk, offset, source):
        start = pl.multiple_of(source * residual_ref.shape[0] + chunk * rows, 16)
        block = shared_ref.at[pl.ds(start, rows)]
        return pltpu.make_async_remote_copy(
            src_ref=block,
            dst_ref=block,
            send_sem=shard_send.at[chunk, offset],
            recv_sem=shard_recv.at[chunk, offset],
            device_id={"seq": (shard + offset) % shards},
            device_id_type=pl.DeviceIdType.MESH,
        )

    def project(chunk):
        here = pl.ds(chunk * rows, rows)
        there = pl.ds(pl.multiple_of(shard * residual_ref.shape[0] + chunk * rows, 16), rows)

        def product(tile):
            columns = pl.ds(pl.multiple_of(tile * kv_width, 128), kv_width)
            return jnp.dot(
                attn_ref[here], weight_ref[:, columns], preferred_element_type=jnp.float32
            ).astype(jnp.bfloat16)

        if chunk == 0:
            for load in loads:
                load.wait()

        @pl.loop(0, 2)
        def _(tile):
            columns = pl.ds(pl.multiple_of(tile * kv_width, 128), kv_width)
            shared_ref[there, columns] = product(tile)

        for offset in range(1, shards):

            @pl.when(shard + offset < shards)
            def _():
                shard_copy(chunk, offset, shard).start()

        @pl.loop(0, query_width // kv_width)
        def _(tile):
            columns = pl.ds(pl.multiple_of(tile * kv_width, 128), kv_width)
            query_ref[here, columns] = product(tile + 2)

    def own_part(chunk, owner):
        return partial_ref[owner, pl.ds(chunk * rows, rows)]

    def sum_step(chunk, step):
        for way in range(2):
            owner = real(way, last - step + place[way])

            @pl.when(place[way] == 0)
            def _():
                stage_ref[way, chunk, step] = own_part(chunk, owner).astype(jnp.bfloat16)
                sum_copy(way, chunk, step).start()

            if step == 0:
                continue

            @pl.when((place[way] <= step) & (place[way] > 0))
            def _():
                sum_copy(way, chunk, step - 1).wait_recv()
                arrived = landed_ref[way, chunk, step - 1].astype(jnp.float32)
                stage_ref[way, chunk, step] = (own_part(chunk, owner) + arrived).astype(
                    jnp.bfloat16
                )
                sum_copy(way, chunk, step).start()

    def finish_sum(chunk):
        here = pl.ds(chunk * rows, rows)
        total_ref[...] = residual_ref[here].astype(jnp.float32) + own_part(chunk, mine)
        for way in range(2):

            @pl.when(place[way] > 0)
            def _():
                sum_copy(way, chunk, last - 1).wait_recv()
                total_ref[...] += landed_ref[way, chunk, last - 1].astype(jnp.float32)

        layer_low = total_ref[...].astype(jnp.bfloat16)
        gathered_ref[mine, here] = layer_low
        layer_ref[here] = layer_low
        for way in range(2):

            @pl.when(place[way] < last)
            def _():
                block_copy(way, chunk, 0, mine).start()

    def forward(chunk, step):
        for way in range(2):
            source = real(way, place[way] - step)

            @pl.when(place[way] >= step)
            def _():
                block_copy(way, chunk, step - 1, source).wait_recv()

            @pl.when((place[way] >= step) & (place[way] < last))
            def _():
                block_copy(way, chunk, step, source).start()

    def normalise(chunk):
        for way in range(2):

            @pl.when(place[way] == last)
            def _():
                block_copy(way, chunk, last - 1, real(way, 0)).wait_recv()

        here = pl.ds(chunk * rows, rows)
        squares = jnp.zeros((rows, 1), jnp.float32)
        for source in range(count):
            block = gathered_ref[source, here].astype(jnp.float32)
            squares += jnp.sum(block * block, axis=1, keepdims=True)
        scale = lax.rsqrt(squares / (count * width) + EPSILON)
        for source in range(count):
            columns = slice(source * width, (source + 1) * width)
            block = gathered_ref[source, here].astype(jnp.float32)
            attn_ref[here, columns] = (block * scale * gain_ref[:, columns]).astype(jnp.bfloat16)

    for tick in range(chunks + 2 * last):
        for index in range(count) if tick < 3 else ():
            if min(index, 2) == tick:
                compute_block(index)
        for chunk in range(chunks):
            stage = tick - chunk
            if 0 <= stage < last:
                sum_step(chunk, stage)
            elif stage == last:
                finish_sum(chunk)
            elif last < stage < 2 * last:
                forward(chunk, stage - last)
        if 0 <= tick - 2 * last < chunks:
            normalise(tick - 2 * last)
            project(tick - 2 * last)

    for chunk in range(chunks):
        for step in range(last):
            for way in range(2):

                @pl.when(place[way] <= step)
                def _():
                    sum_copy(way, chunk, step).wait_send()

                @pl.when((place[way] >= step) & (place[way] < last))
                def _():
                    block_copy(way, chunk, step, real(way, place[way] - step)).wait_send()

        for offset in range(1, shards):

            @pl.when(shard + offset < shards)
            def _():
                shard_copy(chunk, offset, shard).wait_send()

            @pl.when(shard >= offset)
            def _():
                shard_copy(chunk, offset, shard - offset).wait_recv()

    key_value_ref[...] = shared_ref[...]


def line_layer(normed, out_weight, residual, norm_gain, weights, count, shards):
    rows, width = residual.shape
    model_width = width * count
    query_width, kv_width = weights[0].shape[1], weights[1].shape[1]
    chunks = 4 if rows % 64 == 0 else 1
    piece = rows // chunks
    messages = (2, chunks, count - 1)
    vmem = pl.BlockSpec(memory_space=pltpu.VMEM)
    hbm = pl.BlockSpec(memory_space=pltpu.HBM)
    return pl.pallas_call(
        functools.partial(line_kernel, count, shards, chunks),
        out_shape=(
            jax.ShapeDtypeStruct((rows, width), jnp.bfloat16),
            jax.ShapeDtypeStruct((rows, query_width), jnp.bfloat16),
            jax.ShapeDtypeStruct((shards * rows, 2 * kv_width), jnp.bfloat16),
        ),
        in_specs=[vmem, hbm, vmem, vmem, hbm, hbm, hbm],
        out_specs=[vmem] * 3,
        scratch_shapes=[
            pltpu.VMEM((count, out_weight.shape[0], width), jnp.bfloat16),
            pltpu.VMEM((count, rows, width), jnp.float32),
            pltpu.VMEM((model_width, 2 * kv_width + query_width), jnp.bfloat16),
            pltpu.VMEM((rows, model_width), jnp.bfloat16),
            pltpu.VMEM((shards * rows, 2 * kv_width), jnp.bfloat16),
            pltpu.VMEM(messages + (piece, width), jnp.bfloat16),
            pltpu.VMEM(messages + (piece, width), jnp.bfloat16),
            pltpu.VMEM((count, rows, width), jnp.bfloat16),
            pltpu.VMEM((piece, width), jnp.float32),
            pltpu.SemaphoreType.DMA(messages),
            pltpu.SemaphoreType.DMA(messages),
            pltpu.SemaphoreType.DMA(messages),
            pltpu.SemaphoreType.DMA(messages),
            pltpu.SemaphoreType.DMA((chunks, shards)),
            pltpu.SemaphoreType.DMA((chunks, shards)),
            pltpu.SemaphoreType.DMA((3,)),
            pltpu.SemaphoreType.DMA((count,)),
        ],
        compiler_params=pltpu.CompilerParams(
            collective_id=0, has_side_effects=True, vmem_limit_bytes=52 * 1024 * 1024
        ),
    )(normed, out_weight, residual, norm_gain.reshape(1, model_width), *weights)


def attention_kernel(group_size, limits_ref, query_ref, key_ref, value_ref, out_ref):
    rows, count = query_ref.shape[0], key_ref.shape[0]
    limit, first = limits_ref[0], limits_ref[1]
    key_pos = lax.broadcasted_iota(jnp.int32, (rows, count), 1)
    positions = first + lax.broadcasted_iota(jnp.int32, (rows, count), 0)
    allowed = (key_pos <= positions) & (key_pos < limit)
    live = first + lax.broadcasted_iota(jnp.int32, (rows, 1), 0) < limit
    for head in range(group_size):
        columns = slice(head * HEAD_DIM, (head + 1) * HEAD_DIM)
        scores = lax.dot_general(
            query_ref[:, columns],
            key_ref[...],
            (((1,), (1,)), ((), ())),
            preferred_element_type=jnp.float32,
        ) * HEAD_DIM ** (-0.5)
        masked = jnp.where(allowed, scores, NEG_BIG)
        weights = jnp.exp(masked - jnp.max(masked, axis=1, keepdims=True))
        total = jnp.sum(weights, axis=1, keepdims=True)
        accum = jnp.dot(
            weights.astype(jnp.bfloat16), value_ref[...], preferred_element_type=jnp.float32
        )
        head_out = jnp.where(live, accum / jnp.where(live, total, 1.0), 0.0)
        out_ref[:, columns] = head_out.astype(jnp.bfloat16)


def attention(queries, key_value, limit, first):
    rows, count = queries.shape[0], key_value.shape[0]
    kv_local = key_value.shape[1] // (2 * HEAD_DIM)
    group_size = queries.shape[1] // (kv_local * HEAD_DIM)
    wide = (rows, group_size * HEAD_DIM)
    return pl.pallas_call(
        functools.partial(attention_kernel, group_size),
        grid=(kv_local,),
        out_shape=jax.ShapeDtypeStruct(queries.shape, jnp.bfloat16),
        in_specs=[
            pl.BlockSpec(memory_space=pltpu.SMEM),
            pl.BlockSpec(wide, lambda head: (0, head)),
            pl.BlockSpec((count, HEAD_DIM), lambda head: (0, head)),
            pl.BlockSpec((count, HEAD_DIM), lambda head: (0, head + kv_local)),
        ],
        out_specs=pl.BlockSpec(wide, lambda head: (0, head)),
        compiler_params=pltpu.CompilerParams(vmem_limit_bytes=40 * 1024 * 1024),
        cost_estimate=pl.CostEstimate(
            flops=4 * rows * count * queries.shape[1],
            bytes_accessed=4 * queries.size + 2 * key_value.size,
            transcendentals=rows * count * kv_local * group_size,
        ),
    )(jnp.stack([limit, first]), queries, key_value, key_value)


def body(
    length,
    residual,
    ssm_input,
    state_in,
    state_out,
    step_raw,
    decay_rate,
    ssm_gain,
    out_weight,
    norm_gain,
    query_weight,
    key_weight,
    value_weight,
):
    rows = residual.shape[0]
    local_heads = decay_rate.shape[0]
    head_width = ssm_input.shape[1] // local_heads
    seq_index = lax.axis_index("seq")
    limit = length[0]
    positions = seq_index * rows + jnp.arange(rows, dtype=jnp.int32)
    live_rows = positions < limit
    live = live_rows.astype(jnp.float32)
    delta = live[None, :] * jax.nn.softplus(step_raw)
    cumlog = jnp.cumsum(-decay_rate[:, None] * delta, axis=1)
    inputs = ssm_input.astype(jnp.float32).reshape(rows, local_heads, head_width)
    inner = jnp.dot(state_out, state_in.T, preferred_element_type=jnp.float32)
    causal = jnp.arange(rows)[:, None] >= jnp.arange(rows)[None, :]
    spread = cumlog[:, :, None] - cumlog[:, None, :]
    mixing = (
        jnp.where(causal[None], jnp.exp(jnp.where(causal[None], spread, 0.0)), 0.0)
        * inner[None]
        * delta[:, None, :]
    )
    within = jnp.einsum("hts,shp->thp", mixing, inputs, precision=HIGHEST)
    tail = jnp.exp(cumlog[:, -1:] - cumlog) * delta
    local_state = jnp.einsum(
        "hs,shp,sn->hpn", tail, inputs, state_in.astype(jnp.float32), precision=HIGHEST
    )
    incoming = incoming_state(jnp.exp(cumlog[:, -1]), local_state, lax.axis_size("seq"))
    carried = jnp.einsum("hpn,tn->thp", incoming, state_out.astype(jnp.float32), precision=HIGHEST)
    ssm_out = (within + jnp.exp(cumlog).T[:, :, None] * carried) * live[:, None, None]
    mean_square = jnp.mean(ssm_out * ssm_out, axis=2, keepdims=True)
    normed = (
        ssm_out * lax.rsqrt(mean_square + EPSILON) * ssm_gain.reshape(local_heads, head_width)
    ).astype(jnp.bfloat16)
    normed = normed.reshape(rows, local_heads * head_width)
    layer_out, queries, key_value = line_layer(
        normed,
        out_weight,
        residual,
        norm_gain,
        (query_weight, key_weight, value_weight),
        lax.axis_size("head"),
        lax.axis_size("seq"),
    )
    head_out = attention(queries, key_value, limit, seq_index * rows)
    return (layer_out, head_out)


def solution(mesh):
    placed = (
        P("doc"),
        P(("doc", "seq"), "head"),
        P(("doc", "seq"), "head"),
        P(("doc", "seq"), None),
        P(("doc", "seq"), None),
        P(("doc", "head"), "seq"),
        P("head"),
        P("head"),
        P("head", None),
        P(),
        P(None, "head"),
        P(None, "head"),
        P(None, "head"),
    )
    return jax.shard_map(
        body,
        mesh=mesh,
        in_specs=placed,
        out_specs=(P(("doc", "seq"), "head"), P(("doc", "seq"), "head")),
        check_vma=False,
    )
```

```python
import functools

import jax
import jax.numpy as jnp
from jax import lax
from jax.experimental import pallas as pl
from jax.experimental.pallas import tpu as pltpu
from jax.sharding import PartitionSpec as P

HEAD_DIM = 128


EPSILON = 1e-05
NEG_BIG = -1e30
HIGHEST = lax.Precision.HIGHEST


def chain_kernel(
    count, chunks, decay_ref, state_ref, incoming_ref, stage_ref, landed_ref, send_sem, recv_sem
):
    mine = lax.axis_index("seq")
    last = count - 1
    heads = state_ref.shape[0] // chunks
    barrier = pltpu.get_barrier_semaphore()

    def greet(neighbour):
        pl.semaphore_signal(
            barrier, inc=1, device_id={"seq": neighbour}, device_id_type=pl.DeviceIdType.MESH
        )

    @pl.when(mine > 0)
    def _():
        greet(mine - 1)

    @pl.when(mine < last)
    def _():
        greet(mine + 1)

    @pl.when((mine == 0) | (mine == last))
    def _():
        pl.semaphore_wait(barrier, 1)

    @pl.when((mine > 0) & (mine < last))
    def _():
        pl.semaphore_wait(barrier, 2)

    def copy(chunk):
        return pltpu.make_async_remote_copy(
            src_ref=stage_ref.at[chunk],
            dst_ref=landed_ref.at[chunk],
            send_sem=send_sem.at[chunk],
            recv_sem=recv_sem.at[chunk],
            device_id={"seq": mine + 1},
            device_id_type=pl.DeviceIdType.MESH,
        )

    for chunk in range(chunks):
        here = pl.ds(chunk * heads, heads)

        @pl.when(mine == 0)
        def _():
            incoming_ref[here] = jnp.zeros((heads,) + state_ref.shape[1:], jnp.float32)

        @pl.when(mine > 0)
        def _():
            copy(chunk).wait_recv()
            incoming_ref[here] = landed_ref[chunk].astype(jnp.float32)

        @pl.when(mine < last)
        def _():
            for index in range(heads):
                head = chunk * heads + index
                outgoing = decay_ref[head] * incoming_ref[head] + state_ref[head]
                stage_ref[chunk, index] = outgoing.astype(jnp.bfloat16)
            copy(chunk).start()

    for chunk in range(chunks):

        @pl.when(mine < last)
        def _():
            copy(chunk).wait_send()


def incoming_state(block_decay, local_state, count):
    heads, width, states = local_state.shape
    chunks = 4 if heads % 4 == 0 else 1
    slots = (chunks, heads // chunks, width, states)
    return pl.pallas_call(
        functools.partial(chain_kernel, count, chunks),
        out_shape=jax.ShapeDtypeStruct(local_state.shape, jnp.float32),
        in_specs=[
            pl.BlockSpec(memory_space=pltpu.SMEM),
            pl.BlockSpec(memory_space=pltpu.VMEM),
        ],
        out_specs=pl.BlockSpec(memory_space=pltpu.VMEM),
        scratch_shapes=[
            pltpu.VMEM(slots, jnp.bfloat16),
            pltpu.VMEM(slots, jnp.bfloat16),
            pltpu.SemaphoreType.DMA((chunks,)),
            pltpu.SemaphoreType.DMA((chunks,)),
        ],
        compiler_params=pltpu.CompilerParams(collective_id=1, has_side_effects=True),
    )(block_decay, local_state)


def line_kernel(
    count,
    shards,
    chunks,
    normed_ref,
    out_weight_ref,
    residual_ref,
    gain_ref,
    query_weight_ref,
    key_weight_ref,
    value_weight_ref,
    layer_ref,
    query_ref,
    key_value_ref,
    block_weight_ref,
    partial_ref,
    weight_ref,
    attn_ref,
    shared_ref,
    stage_ref,
    landed_ref,
    gathered_ref,
    total_ref,
    sum_send,
    sum_recv,
    copy_send,
    copy_recv,
    shard_send,
    shard_recv,
    weight_sem,
    block_sem,
):
    mine = lax.axis_index("head")
    last = count - 1
    width = residual_ref.shape[1]
    rows = residual_ref.shape[0] // chunks
    place = (mine, last - mine)

    shard = lax.axis_index("seq")
    query_width = query_ref.shape[1]
    kv_width = key_weight_ref.shape[1]
    starts = (0, kv_width, 2 * kv_width)
    loads = [
        pltpu.make_async_copy(
            source, weight_ref.at[:, pl.ds(start, source.shape[1])], weight_sem.at[index]
        )
        for index, (source, start) in enumerate(
            zip((key_weight_ref, value_weight_ref, query_weight_ref), starts)
        )
    ]

    def ordered(index):
        return jnp.where(2 * mine < count, last - index, index)

    def block_load(index):
        columns = pl.ds(pl.multiple_of(ordered(index) * width, 128), width)
        return pltpu.make_async_copy(
            out_weight_ref.at[:, columns], block_weight_ref.at[index], block_sem.at[index]
        )

    for index in range(count):
        block_load(index).start()
    for load in loads:
        load.start()

    def compute_block(index):
        block_load(index).wait()
        tile = min(width, 256)

        @pl.loop(0, width // tile)
        def _(step):
            columns = pl.ds(pl.multiple_of(step * tile, 128), tile)
            partial_ref[ordered(index), :, columns] = jnp.dot(
                normed_ref[...],
                block_weight_ref[index, :, columns],
                preferred_element_type=jnp.float32,
            )

    barrier = pltpu.get_barrier_semaphore()

    def greet(neighbour):
        pl.semaphore_signal(
            barrier, inc=1, device_id={"head": neighbour}, device_id_type=pl.DeviceIdType.MESH
        )

    @pl.when(mine > 0)
    def _():
        greet(mine - 1)

    @pl.when(mine < last)
    def _():
        greet(mine + 1)

    for offset in range(1, shards):
        other = (shard + offset) % shards
        pl.semaphore_signal(
            barrier, inc=1, device_id={"seq": other}, device_id_type=pl.DeviceIdType.MESH
        )

    @pl.when((mine == 0) | (mine == last))
    def _():
        pl.semaphore_wait(barrier, shards)

    @pl.when((mine > 0) & (mine < last))
    def _():
        pl.semaphore_wait(barrier, shards + 1)

    for other in range(shards):

        @pl.when(other > shard)
        def _():
            shared_ref[pl.ds(other * residual_ref.shape[0], residual_ref.shape[0])] = jnp.zeros(
                (residual_ref.shape[0], 2 * kv_width), jnp.bfloat16
            )

    def neighbour(way):
        return mine + 1 if way == 0 else mine - 1

    def real(way, position):
        return position if way == 0 else last - position

    def sum_copy(way, chunk, step):
        return pltpu.make_async_remote_copy(
            src_ref=stage_ref.at[way, chunk, step],
            dst_ref=landed_ref.at[way, chunk, step],
            send_sem=sum_send.at[way, chunk, step],
            recv_sem=sum_recv.at[way, chunk, step],
            device_id={"head": neighbour(way)},
            device_id_type=pl.DeviceIdType.MESH,
        )

    def block_copy(way, chunk, step, source):
        block = gathered_ref.at[source, pl.ds(chunk * rows, rows)]
        return pltpu.make_async_remote_copy(
            src_ref=block,
            dst_ref=block,
            send_sem=copy_send.at[way, chunk, step],
            recv_sem=copy_recv.at[way, chunk, step],
            device_id={"head": neighbour(way)},
            device_id_type=pl.DeviceIdType.MESH,
        )

    def shard_copy(chunk, offset, source):
        start = pl.multiple_of(source * residual_ref.shape[0] + chunk * rows, 16)
        block = shared_ref.at[pl.ds(start, rows)]
        return pltpu.make_async_remote_copy(
            src_ref=block,
            dst_ref=block,
            send_sem=shard_send.at[chunk, offset],
            recv_sem=shard_recv.at[chunk, offset],
            device_id={"seq": (shard + offset) % shards},
            device_id_type=pl.DeviceIdType.MESH,
        )

    def project(chunk):
        here = pl.ds(chunk * rows, rows)
        there = pl.ds(pl.multiple_of(shard * residual_ref.shape[0] + chunk * rows, 16), rows)

        def product(tile):
            columns = pl.ds(pl.multiple_of(tile * kv_width, 128), kv_width)
            return jnp.dot(
                attn_ref[here], weight_ref[:, columns], preferred_element_type=jnp.float32
            ).astype(jnp.bfloat16)

        if chunk == 0:
            for load in loads:
                load.wait()

        @pl.loop(0, 2)
        def _(tile):
            columns = pl.ds(pl.multiple_of(tile * kv_width, 128), kv_width)
            shared_ref[there, columns] = product(tile)

        for offset in range(1, shards):

            @pl.when(shard + offset < shards)
            def _():
                shard_copy(chunk, offset, shard).start()

        @pl.loop(0, query_width // kv_width)
        def _(tile):
            columns = pl.ds(pl.multiple_of(tile * kv_width, 128), kv_width)
            query_ref[here, columns] = product(tile + 2)

    def own_part(chunk, owner):
        return partial_ref[owner, pl.ds(chunk * rows, rows)]

    def sum_step(chunk, step):
        for way in range(2):
            owner = real(way, last - step + place[way])

            @pl.when(place[way] == 0)
            def _():
                stage_ref[way, chunk, step] = own_part(chunk, owner).astype(jnp.bfloat16)
                sum_copy(way, chunk, step).start()

            if step == 0:
                continue

            @pl.when((place[way] <= step) & (place[way] > 0))
            def _():
                sum_copy(way, chunk, step - 1).wait_recv()
                arrived = landed_ref[way, chunk, step - 1].astype(jnp.float32)
                stage_ref[way, chunk, step] = (own_part(chunk, owner) + arrived).astype(
                    jnp.bfloat16
                )
                sum_copy(way, chunk, step).start()

    def finish_sum(chunk):
        here = pl.ds(chunk * rows, rows)
        total_ref[...] = residual_ref[here].astype(jnp.float32) + own_part(chunk, mine)
        for way in range(2):

            @pl.when(place[way] > 0)
            def _():
                sum_copy(way, chunk, last - 1).wait_recv()
                total_ref[...] += landed_ref[way, chunk, last - 1].astype(jnp.float32)

        layer_low = total_ref[...].astype(jnp.bfloat16)
        gathered_ref[mine, here] = layer_low
        layer_ref[here] = layer_low
        for way in range(2):

            @pl.when(place[way] < last)
            def _():
                block_copy(way, chunk, 0, mine).start()

    def forward(chunk, step):
        for way in range(2):
            source = real(way, place[way] - step)

            @pl.when(place[way] >= step)
            def _():
                block_copy(way, chunk, step - 1, source).wait_recv()

            @pl.when((place[way] >= step) & (place[way] < last))
            def _():
                block_copy(way, chunk, step, source).start()

    def normalise(chunk):
        for way in range(2):

            @pl.when(place[way] == last)
            def _():
                block_copy(way, chunk, last - 1, real(way, 0)).wait_recv()

        here = pl.ds(chunk * rows, rows)
        squares = jnp.zeros((rows, 1), jnp.float32)
        for source in range(count):
            block = gathered_ref[source, here].astype(jnp.float32)
            squares += jnp.sum(block * block, axis=1, keepdims=True)
        scale = lax.rsqrt(squares / (count * width) + EPSILON)
        for source in range(count):
            columns = slice(source * width, (source + 1) * width)
            block = gathered_ref[source, here].astype(jnp.float32)
            attn_ref[here, columns] = (block * scale * gain_ref[:, columns]).astype(jnp.bfloat16)

    for tick in range(chunks + 2 * last):
        for index in range(count) if tick < 3 else ():
            if min(index, 2) == tick:
                compute_block(index)
        for chunk in reversed(range(chunks)):
            stage = tick - chunk
            if 0 <= stage < last:
                sum_step(chunk, stage)
            elif stage == last:
                finish_sum(chunk)
            elif last < stage < 2 * last:
                forward(chunk, stage - last)
        if 0 <= tick - 2 * last < chunks:
            normalise(tick - 2 * last)
            project(tick - 2 * last)

    for chunk in range(chunks):
        for step in range(last):
            for way in range(2):

                @pl.when(place[way] <= step)
                def _():
                    sum_copy(way, chunk, step).wait_send()

                @pl.when((place[way] >= step) & (place[way] < last))
                def _():
                    block_copy(way, chunk, step, real(way, place[way] - step)).wait_send()

        for offset in range(1, shards):

            @pl.when(shard + offset < shards)
            def _():
                shard_copy(chunk, offset, shard).wait_send()

            @pl.when(shard >= offset)
            def _():
                shard_copy(chunk, offset, shard - offset).wait_recv()

    key_value_ref[...] = shared_ref[...]


def line_layer(normed, out_weight, residual, norm_gain, weights, count, shards):
    rows, width = residual.shape
    model_width = width * count
    query_width, kv_width = weights[0].shape[1], weights[1].shape[1]
    chunks = 4 if rows % 64 == 0 else 1
    piece = rows // chunks
    messages = (2, chunks, count - 1)
    vmem = pl.BlockSpec(memory_space=pltpu.VMEM)
    hbm = pl.BlockSpec(memory_space=pltpu.HBM)
    return pl.pallas_call(
        functools.partial(line_kernel, count, shards, chunks),
        out_shape=(
            jax.ShapeDtypeStruct((rows, width), jnp.bfloat16),
            jax.ShapeDtypeStruct((rows, query_width), jnp.bfloat16),
            jax.ShapeDtypeStruct((shards * rows, 2 * kv_width), jnp.bfloat16),
        ),
        in_specs=[vmem, hbm, vmem, vmem, hbm, hbm, hbm],
        out_specs=[vmem] * 3,
        scratch_shapes=[
            pltpu.VMEM((count, out_weight.shape[0], width), jnp.bfloat16),
            pltpu.VMEM((count, rows, width), jnp.float32),
            pltpu.VMEM((model_width, 2 * kv_width + query_width), jnp.bfloat16),
            pltpu.VMEM((rows, model_width), jnp.bfloat16),
            pltpu.VMEM((shards * rows, 2 * kv_width), jnp.bfloat16),
            pltpu.VMEM(messages + (piece, width), jnp.bfloat16),
            pltpu.VMEM(messages + (piece, width), jnp.bfloat16),
            pltpu.VMEM((count, rows, width), jnp.bfloat16),
            pltpu.VMEM((piece, width), jnp.float32),
            pltpu.SemaphoreType.DMA(messages),
            pltpu.SemaphoreType.DMA(messages),
            pltpu.SemaphoreType.DMA(messages),
            pltpu.SemaphoreType.DMA(messages),
            pltpu.SemaphoreType.DMA((chunks, shards)),
            pltpu.SemaphoreType.DMA((chunks, shards)),
            pltpu.SemaphoreType.DMA((3,)),
            pltpu.SemaphoreType.DMA((count,)),
        ],
        compiler_params=pltpu.CompilerParams(
            collective_id=0, has_side_effects=True, vmem_limit_bytes=52 * 1024 * 1024
        ),
    )(normed, out_weight, residual, norm_gain.reshape(1, model_width), *weights)


def attention_kernel(group_size, limits_ref, query_ref, key_ref, value_ref, out_ref):
    rows, count = query_ref.shape[0], key_ref.shape[0]
    limit, first = limits_ref[0], limits_ref[1]
    key_pos = lax.broadcasted_iota(jnp.int32, (rows, count), 1)
    positions = first + lax.broadcasted_iota(jnp.int32, (rows, count), 0)
    allowed = (key_pos <= positions) & (key_pos < limit)
    live = first + lax.broadcasted_iota(jnp.int32, (rows, 1), 0) < limit
    for head in range(group_size):
        columns = slice(head * HEAD_DIM, (head + 1) * HEAD_DIM)
        scores = lax.dot_general(
            query_ref[:, columns],
            key_ref[...],
            (((1,), (1,)), ((), ())),
            preferred_element_type=jnp.float32,
        ) * HEAD_DIM ** (-0.5)
        masked = jnp.where(allowed, scores, NEG_BIG)
        weights = jnp.exp(masked - jnp.max(masked, axis=1, keepdims=True))
        total = jnp.sum(weights, axis=1, keepdims=True)
        accum = jnp.dot(
            weights.astype(jnp.bfloat16), value_ref[...], preferred_element_type=jnp.float32
        )
        head_out = jnp.where(live, accum / jnp.where(live, total, 1.0), 0.0)
        out_ref[:, columns] = head_out.astype(jnp.bfloat16)


def attention(queries, key_value, limit, first):
    rows, count = queries.shape[0], key_value.shape[0]
    kv_local = key_value.shape[1] // (2 * HEAD_DIM)
    group_size = queries.shape[1] // (kv_local * HEAD_DIM)
    wide = (rows, group_size * HEAD_DIM)
    return pl.pallas_call(
        functools.partial(attention_kernel, group_size),
        grid=(kv_local,),
        out_shape=jax.ShapeDtypeStruct(queries.shape, jnp.bfloat16),
        in_specs=[
            pl.BlockSpec(memory_space=pltpu.SMEM),
            pl.BlockSpec(wide, lambda head: (0, head)),
            pl.BlockSpec((count, HEAD_DIM), lambda head: (0, head)),
            pl.BlockSpec((count, HEAD_DIM), lambda head: (0, head + kv_local)),
        ],
        out_specs=pl.BlockSpec(wide, lambda head: (0, head)),
        compiler_params=pltpu.CompilerParams(vmem_limit_bytes=40 * 1024 * 1024),
        cost_estimate=pl.CostEstimate(
            flops=4 * rows * count * queries.shape[1],
            bytes_accessed=4 * queries.size + 2 * key_value.size,
            transcendentals=rows * count * kv_local * group_size,
        ),
    )(jnp.stack([limit, first]), queries, key_value, key_value)


def body(
    length,
    residual,
    ssm_input,
    state_in,
    state_out,
    step_raw,
    decay_rate,
    ssm_gain,
    out_weight,
    norm_gain,
    query_weight,
    key_weight,
    value_weight,
):
    rows = residual.shape[0]
    local_heads = decay_rate.shape[0]
    head_width = ssm_input.shape[1] // local_heads
    seq_index = lax.axis_index("seq")
    limit = length[0]
    positions = seq_index * rows + jnp.arange(rows, dtype=jnp.int32)
    live_rows = positions < limit
    live = live_rows.astype(jnp.float32)
    delta = live[None, :] * jax.nn.softplus(step_raw)
    cumlog = jnp.cumsum(-decay_rate[:, None] * delta, axis=1)
    inputs = ssm_input.astype(jnp.float32).reshape(rows, local_heads, head_width)
    inner = jnp.dot(state_out, state_in.T, preferred_element_type=jnp.float32)
    causal = jnp.arange(rows)[:, None] >= jnp.arange(rows)[None, :]
    spread = cumlog[:, :, None] - cumlog[:, None, :]
    mixing = (
        jnp.where(causal[None], jnp.exp(jnp.where(causal[None], spread, 0.0)), 0.0)
        * inner[None]
        * delta[:, None, :]
    )
    within = jnp.einsum("hts,shp->thp", mixing, inputs, precision=HIGHEST)
    tail = jnp.exp(cumlog[:, -1:] - cumlog) * delta
    local_state = jnp.einsum(
        "hs,shp,sn->hpn", tail, inputs, state_in.astype(jnp.float32), precision=HIGHEST
    )
    incoming = incoming_state(jnp.exp(cumlog[:, -1]), local_state, lax.axis_size("seq"))
    carried = jnp.einsum("hpn,tn->thp", incoming, state_out.astype(jnp.float32), precision=HIGHEST)
    ssm_out = (within + jnp.exp(cumlog).T[:, :, None] * carried) * live[:, None, None]
    mean_square = jnp.mean(ssm_out * ssm_out, axis=2, keepdims=True)
    normed = (
        ssm_out * lax.rsqrt(mean_square + EPSILON) * ssm_gain.reshape(local_heads, head_width)
    ).astype(jnp.bfloat16)
    normed = normed.reshape(rows, local_heads * head_width)
    layer_out, queries, key_value = line_layer(
        normed,
        out_weight,
        residual,
        norm_gain,
        (query_weight, key_weight, value_weight),
        lax.axis_size("head"),
        lax.axis_size("seq"),
    )
    head_out = attention(queries, key_value, limit, seq_index * rows)
    return (layer_out, head_out)


def solution(mesh):
    placed = (
        P("doc"),
        P(("doc", "seq"), "head"),
        P(("doc", "seq"), "head"),
        P(("doc", "seq"), None),
        P(("doc", "seq"), None),
        P(("doc", "head"), "seq"),
        P("head"),
        P("head"),
        P("head", None),
        P(),
        P(None, "head"),
        P(None, "head"),
        P(None, "head"),
    )
    return jax.shard_map(
        body,
        mesh=mesh,
        in_specs=placed,
        out_specs=(P(("doc", "seq"), "head"), P(("doc", "seq"), "head")),
        check_vma=False,
    )
```
